32 devices in a mesh: ka: 16 (over z, y, x), occ: 2 (over core).
Axes of the slice: x: 2, y: 2, z: 4, core: 2. Of those that a mesh axis runs over, the one named last changes fastest.
Arguments:
- factors: bfloat16 [32, 2, 192, 2, 768], P('ka'), may hold values from -0.23925781 to 0.23925781
- occupied_energy: float32 [2], replicated, may hold values from -2 to -0.5
- virtual_energy: bfloat16 [32, 192], P('ka'), may hold values from 0.5 to 3
- conserve: int32 [32, 2], P('ka'), may hold values from 0 to 31, as said below
- pair_lists: int32 [2, 4, 2], P(None, 'occ'), may hold values from 0 to 1, as said below
Outputs:
- density: float32 [32, 192, 2, 192], P('ka', 'occ')
The draws below stay inside these ranges and needn't reach their ends.
Inputs may be any that keep to these rules, and one draw needn't show every extreme that they name: For a momentum ka among the 2 momenta of block d (momenta d * 2 to d * 2 + 1), (32 - conserve[ka, r]) mod 32 lies in block (d - r - 1) mod 16; the 2 momenta of one block name different momenta in each round. `pair_lists`: each entry is an ordered pair (i, j) of occupied orbitals; every round begins with the pairs (0, 0) and (1, 1); within a round no ordered pair repeats (4 of the 4 ordered pairs appear).
All inputs are finite; a program needn't handle non-finite values.
Results may differ from the reference program's by a relative error of at most 0.00082.
Values may be sent and summed in bfloat16 or wider, within the bound.
A program may use at most 128 MiB of HBM per device.

```python
import jax
import jax.numpy as jnp
from jax import lax

NV = 192
NAUX = 768
KA_DEV = 2
ROUNDS = 2
NK = 32
NOCC = 2
NPAIRS = 4


def draw_conserve(key, part):
    groups = NK // KA_DEV
    row_keys = jax.random.split(jax.random.fold_in(key, 7), groups * ROUNDS)
    orders = jax.vmap(lambda single: jax.random.permutation(single, KA_DEV))(row_keys)
    orders = orders.reshape(groups, ROUNDS, KA_DEV).transpose(0, 2, 1).astype(jnp.int32)
    device = jnp.arange(groups, dtype=jnp.int32)[:, None, None]
    round_ids = jnp.arange(ROUNDS, dtype=jnp.int32)[None, None, :]
    source = (device - round_ids - 1) % groups
    mirror = source * KA_DEV + orders
    return ((NK - mirror) % NK).reshape(NK, ROUNDS).astype(jnp.int32)


def draw_pair_lists(key, part):
    square = NOCC * NOCC
    round_keys = jax.random.split(jax.random.fold_in(key, 11), ROUNDS)
    middle = jax.vmap(lambda single: jax.random.permutation(single, square - 2))(round_keys).astype(jnp.int32) + 1
    ends = jnp.broadcast_to(jnp.array([0, square - 1], dtype=jnp.int32)[None, :], (ROUNDS, 2))
    orders = jnp.concatenate([ends, middle], axis=1)
    positions = jnp.arange(NPAIRS, dtype=jnp.int32)
    picked = orders[:, positions % square]
    extra = jax.random.randint(jax.random.fold_in(key, 13), (ROUNDS, NPAIRS), 0, square).astype(jnp.int32)
    flat = jnp.where(positions[None, :] < square, picked, extra)
    leading = flat // NOCC
    trailing = flat % NOCC
    return jnp.stack([leading, trailing], axis=-1).astype(jnp.int32)


def block_levels(rng, dims, cuts, smallest, largest):
    def one(position, parts):
        steps = jax.random.uniform(jax.random.fold_in(jax.random.fold_in(rng, 6), position), (parts,), jnp.float32, smallest / len(cuts), largest / len(cuts))
        return jnp.repeat(jnp.exp(steps), dims[position] // parts).reshape((-1,) + (1,) * (len(dims) - position - 1))

    gain = one(*cuts[0])
    for cut in cuts[1:]:
        gain = gain * one(*cut)
    return gain


def normal_values(own_key, extent, spread, most, cuts=(), kind=jnp.bfloat16):
    entries = spread * jax.random.normal(own_key, extent, jnp.float32)
    if cuts:
        entries = entries * block_levels(own_key, extent, cuts, -0.22, 0.18)
    return jnp.clip(entries, -most, most).astype(kind)


def setup_inputs(seed: int = 0) -> dict:
    seeds = jax.random.split(jax.random.key(seed), 6)
    factors = normal_values(seeds[0], (NK, NOCC, NV, 2, NAUX), 0.04, 0.23925781, ((0, 16),))
    occupied_energy = jnp.clip(jax.random.uniform(seeds[1], (NOCC,), jnp.float32, -2.0, -0.5), -2.0, -0.5)
    virtual_energy = jnp.clip(0.5 + 2.5 * jax.random.uniform(seeds[2], (NK, NV), jnp.float32) ** block_levels(seeds[2], (NK, NV), ((0, 16),), -0.2, 0.2), 0.5, 3.0).astype(jnp.bfloat16)
    conserve = draw_conserve(jax.random.fold_in(seeds[5], 71), 0)
    pair_lists = draw_pair_lists(jax.random.fold_in(seeds[5], 71), 0)
    return {"factors": factors, "occupied_energy": occupied_energy, "virtual_energy": virtual_energy, "conserve": conserve, "pair_lists": pair_lists}


def build_mates(received, auxiliary):
    real_part = received[..., :auxiliary]
    imaginary = received[..., auxiliary:]
    turned = jnp.concatenate([-imaginary, real_part], axis=-1)
    return jnp.concatenate([received, turned], axis=-2)


def amplitude(left_rows, mate_rows, energy_left, energy_right, occupied_sum):
    values = lax.dot_general(left_rows, mate_rows, (((1,), (1,)), ((), ())), preferred_element_type=jnp.float32)
    denominator = energy_left[:, None] + energy_right[None, :] - occupied_sum
    return values / jnp.concatenate([denominator, denominator], axis=1)


def density_term(amplitudes, swapped):
    virtuals = amplitudes.shape[0]
    combined = (2.0 * amplitudes - swapped).astype(jnp.bfloat16)
    rounded = amplitudes.astype(jnp.bfloat16)
    turned = jnp.concatenate([-rounded[:, virtuals:], rounded[:, :virtuals]], axis=1)
    stacked = jnp.concatenate([rounded, turned], axis=0)
    return lax.dot_general(combined, stacked, (((1,), (1,)), ((), ())), preferred_element_type=jnp.float32)


def pair_term(own_block, mate_block, energy_left, energy_right, occupied_energy, pair_row):
    leading = pair_row[0]
    trailing = pair_row[1]
    occupied_sum = occupied_energy[leading] + occupied_energy[trailing]
    amplitudes = amplitude(own_block[leading], mate_block[trailing], energy_left, energy_right, occupied_sum)
    swapped = amplitude(own_block[trailing], mate_block[leading], energy_left, energy_right, occupied_sum)
    return density_term(amplitudes, swapped)


def reference(factors, occupied_energy, virtual_energy, conserve, pair_lists):
    momentum_count = factors.shape[0]
    orbitals = factors.shape[1]
    virtuals = factors.shape[2]
    auxiliary = factors.shape[4]
    stacked = factors.reshape(momentum_count, orbitals, virtuals, 2 * auxiliary)
    energies = virtual_energy.astype(jnp.float32)

    def one_momentum(moment):
        own_block = stacked[moment]
        energy_left = energies[moment]
        running = jnp.zeros((virtuals, 2 * virtuals), jnp.float32)
        for round_index in range(conserve.shape[1]):
            mirror = ((momentum_count - conserve[moment, round_index]) % momentum_count).astype(jnp.int32)
            mate_block = build_mates(stacked[mirror], auxiliary)
            energy_right = energies[mirror]

            def add_pair(partial_sum, pair_row):
                term = pair_term(own_block, mate_block, energy_left, energy_right, occupied_energy, pair_row)
                return partial_sum + term, None

            running, ignored = lax.scan(add_pair, running, pair_lists[round_index])
        return running.reshape(virtuals, 2, virtuals)

    return lax.map(one_momentum, jnp.arange(momentum_count, dtype=jnp.int32))
```

```python
import functools

import jax
import jax.numpy as jnp
from jax import lax
from jax.experimental import pallas as pl
from jax.experimental.pallas import tpu as pltpu
from jax.sharding import PartitionSpec as P

LANES = 128
BAND = 64
STEP = 16
PIECE = 8


def from_behind(array, axis, by):
    size = lax.axis_size(axis)
    return lax.ppermute(array, axis, [(i, (i + by) % size) for i in range(size)])


def build_mates(received, auxiliary):
    real_part = received[..., :auxiliary]
    imaginary = received[..., auxiliary:]
    turned = jnp.concatenate([-imaginary, real_part], axis=-1)
    return jnp.concatenate([received, turned], axis=-2)


def amplitude(left_rows, mate_rows, energy_left, energy_right, occupied_sum):
    values = lax.dot_general(
        left_rows, mate_rows, (((1,), (1,)), ((), ())), preferred_element_type=jnp.float32
    )
    denominator = energy_left[:, None] + energy_right[None, :] - occupied_sum
    return values / jnp.concatenate([denominator, denominator], axis=1)


def density_term(amplitudes, swapped):
    virtuals = amplitudes.shape[0]
    combined = (2.0 * amplitudes - swapped).astype(jnp.bfloat16)
    rounded = amplitudes.astype(jnp.bfloat16)
    turned = jnp.concatenate([-rounded[:, virtuals:], rounded[:, :virtuals]], axis=1)
    stacked = jnp.concatenate([rounded, turned], axis=0)
    return lax.dot_general(
        combined, stacked, (((1,), (1,)), ((), ())), preferred_element_type=jnp.float32
    )


def pair_term(own_block, mate_block, energy_left, energy_right, occupied_energy, pair_row):
    leading = pair_row[0]
    trailing = pair_row[1]
    occupied_sum = occupied_energy[leading] + occupied_energy[trailing]
    amplitudes = amplitude(
        own_block[leading], mate_block[trailing], energy_left, energy_right, occupied_sum
    )
    swapped = amplitude(
        own_block[trailing], mate_block[leading], energy_left, energy_right, occupied_sum
    )
    return density_term(amplitudes, swapped)


def general(factors, occupied_energy, virtual_energy, conserve, pair_lists):
    momenta = factors.shape[0]
    orbitals = factors.shape[1]
    virtuals = factors.shape[2]
    auxiliary = factors.shape[4]
    own = factors.reshape(momenta, orbitals, virtuals, 2 * auxiliary)
    energy_own = virtual_energy.astype(jnp.float32)
    density = jnp.zeros((momenta, virtuals, 2 * virtuals), jnp.float32)
    for round_index in range(conserve.shape[1]):
        portion = orbitals // lax.axis_size("occ")
        portion_block = lax.dynamic_slice_in_dim(
            factors, lax.axis_index("occ") * portion, portion, 1
        )
        shifted, energy_mate = from_behind((portion_block, virtual_energy), "ka", round_index + 1)
        received = lax.all_gather(shifted, "occ", axis=1, tiled=True)
        mates = build_mates(received.reshape(momenta, orbitals, virtuals, 2 * auxiliary), auxiliary)
        energy_mate = energy_mate.astype(jnp.float32)
        for local_index in range(momenta):
            chosen = (momenta - conserve[local_index, round_index] % momenta) % momenta
            mate_block = lax.dynamic_index_in_dim(mates, chosen, 0, keepdims=False)
            energy_right = lax.dynamic_index_in_dim(energy_mate, chosen, 0, keepdims=False)
            own_block = own[local_index]
            energy_left = energy_own[local_index]

            def add_pair(partial_sum, pair_row):
                term = pair_term(
                    own_block, mate_block, energy_left, energy_right, occupied_energy, pair_row
                )
                return (partial_sum + term, None)

            running, ignored = lax.scan(add_pair, density[local_index], pair_lists[round_index])
            density = density.at[local_index].set(running)
    shaped = density.reshape(momenta, virtuals, 2, virtuals)
    return lax.psum_scatter(shaped, "occ", scatter_dimension=1, tiled=True)


def fused_kernel(
    ring, virtuals, auxiliary,
    conserve_hbm, occupied_hbm, energy_hbm, factors_ref, out_ref,
    conserve_ref, occupied_ref, energy_ref, own_raw, mate_raw, own, mate, energy_in, energy_left, inverse, products, total, outgoing, incoming,
    small_sem, own_sem, far_send, far_recv, near_send, near_recv,
    energy_send, energy_recv, swap_send, swap_recv,
):
    mesh_id = pl.DeviceIdType.MESH
    me = lax.axis_index("ka")
    core = lax.axis_index("occ")
    other = 1 - core
    odd = lax.rem(me, 2)
    half = virtuals // 2
    pieces = virtuals // PIECE
    steps = virtuals // STEP
    bands = virtuals // BAND
    per_step = STEP // PIECE
    per_band = BAND // STEP
    tiles = pl.cdiv(virtuals, LANES)
    stride = 2 * tiles

    def at(step):
        return lax.rem(me + step + ring, ring)

    near = at(1 - 2 * odd)

    def own_copy(momentum, index):
        return pltpu.make_async_copy(
            factors_ref.at[momentum], own_raw.at[momentum], own_sem.at[index]
        )

    def small_copies():
        return (
            pltpu.make_async_copy(conserve_hbm, conserve_ref, small_sem.at[0]),
            pltpu.make_async_copy(occupied_hbm, occupied_ref, small_sem.at[1]),
            pltpu.make_async_copy(energy_hbm, energy_ref, small_sem.at[2]),
        )

    barrier = pltpu.get_barrier_semaphore()
    for place in ((at(-2), core), (near, core), (me, other)):
        pl.semaphore_signal(barrier, inc=1, device_id=place, device_id_type=mesh_id)
    own_copy(core, 0).start()
    for copy in small_copies():
        copy.start()
    own_copy(other, 1).start()

    def piece_rows(piece):
        return pl.ds(pl.multiple_of(piece * PIECE, PIECE), PIECE)

    def step_rows(step):
        return pl.ds(pl.multiple_of(step * STEP, STEP), STEP)

    def far_copy(piece):
        return pltpu.make_async_remote_copy(
            src_ref=own_raw.at[core, :, piece_rows(piece)],
            dst_ref=mate_raw.at[1, :, piece_rows(piece)],
            send_sem=far_send.at[piece], recv_sem=far_recv.at[piece],
            device_id=(at(2), core), device_id_type=mesh_id,
        )

    def near_copy(piece, relay):
        source = mate_raw.at[1] if relay else own_raw.at[core]
        return pltpu.make_async_remote_copy(
            src_ref=source.at[:, piece_rows(piece)],
            dst_ref=mate_raw.at[0, :, piece_rows(piece)],
            send_sem=near_send.at[piece], recv_sem=near_recv.at[piece],
            device_id=(near, core), device_id_type=mesh_id,
        )

    def energy_far():
        return pltpu.make_async_remote_copy(
            src_ref=energy_ref, dst_ref=energy_in.at[1],
            send_sem=energy_send.at[1], recv_sem=energy_recv.at[1],
            device_id=(at(2), core), device_id_type=mesh_id,
        )

    def energy_near(relay):
        return pltpu.make_async_remote_copy(
            src_ref=energy_in.at[1] if relay else energy_ref, dst_ref=energy_in.at[0],
            send_sem=energy_send.at[0], recv_sem=energy_recv.at[0],
            device_id=(near, core), device_id_type=mesh_id,
        )

    own_copy(core, 0).wait()
    pl.semaphore_wait(barrier, 3)

    def send_piece(piece, carry):
        far_copy(piece).start()

        @pl.when(odd == 0)
        def _():
            near_copy(piece, False).start()

        return carry

    lax.fori_loop(0, 2, send_piece, 0)
    for copy in small_copies():
        copy.wait()
    energy_far().start()

    @pl.when(odd == 0)
    def _():
        energy_near(False).start()

    lax.fori_loop(2, pieces, send_piece, 0)

    chosen = []
    for slot in range(2):
        mirror = lax.rem(2 - lax.rem(conserve_ref[0, slot], 2), 2)
        chosen.append(jnp.where(mirror == core, 0, 1))

    own_copy(other, 1).wait()

    def forward(piece):
        far_copy(piece).wait_recv()

        @pl.when(odd == 1)
        def _():
            near_copy(piece, True).start()

    def shape_own(step, carry):
        for momentum in range(2):
            for orbital in range(2):
                row = pl.ds(pl.multiple_of(orbital * virtuals + step * STEP, STEP), STEP)
                for part in range(2):
                    own[momentum, row, pl.ds(part * auxiliary, auxiliary)] = own_raw[
                        momentum, orbital, step_rows(step), part, :
                    ]
        return carry

    def shape_mate(slot, step):
        band = step // per_band
        for orbital in range(2):
            real = mate_raw[slot, orbital, step_rows(step), 0, :]
            imaginary = mate_raw[slot, orbital, step_rows(step), 1, :]
            first = orbital * 2 * BAND + lax.rem(step, per_band) * STEP
            plain = pl.ds(pl.multiple_of(first, STEP), STEP)
            turned = pl.ds(pl.multiple_of(first + BAND, STEP), STEP)
            mate[slot, band, plain, pl.ds(0, auxiliary)] = real
            mate[slot, band, plain, pl.ds(auxiliary, auxiliary)] = imaginary
            mate[slot, band, turned, pl.ds(0, auxiliary)] = -imaginary
            mate[slot, band, turned, pl.ds(auxiliary, auxiliary)] = real

    def shape_energies():
        sums = [occupied_ref[0] + occupied_ref[0], occupied_ref[0] + occupied_ref[1]]
        sums.append(occupied_ref[1] + occupied_ref[1])
        diagonal = lax.broadcasted_iota(
            jnp.int32, (virtuals, virtuals), 0
        ) == lax.broadcasted_iota(jnp.int32, (virtuals, virtuals), 1)
        mine = energy_ref[...].astype(jnp.float32)
        for momentum in range(2):
            spread = jnp.where(diagonal, mine[momentum : momentum + 1, :], 0.0)
            column = jnp.sum(spread, axis=1, keepdims=True)
            energy_left[momentum] = jnp.broadcast_to(column, (virtuals, LANES))
        energy_near(False).wait_recv()
        for slot in range(2):
            theirs = energy_in[slot].astype(jnp.float32)
            theirs = jnp.where(core == 0, theirs[0:1, :], theirs[1:2, :])
            for band in range(bands):
                part = theirs[:, band * BAND : (band + 1) * BAND]
                row = jnp.concatenate([part, part], axis=1)
                base = energy_left[chosen[slot]] + row
                for kind in range(3):
                    inverse[slot, band, kind] = 1.0 / (base - sums[kind])

    sign = jnp.where(lax.broadcasted_iota(jnp.int32, (virtuals, LANES), 1) < BAND, -1.0, 1.0)

    def add_band(slot, band):
        momentum = jnp.where(slot == 1, chosen[1], chosen[0])
        products[...] = lax.dot_general(
            own[momentum], mate[slot, band], (((1,), (1,)), ((), ())),
            preferred_element_type=jnp.float32,
        )
        amplitudes = {}
        for i in range(2):
            for j in range(2):
                value = products[i * virtuals : (i + 1) * virtuals, j * LANES : (j + 1) * LANES]
                amplitudes[i, j] = value * inverse[slot, band, i + j]
        combined, rounded, turned = [], [], []
        for i in range(2):
            for j in range(2):
                this = amplitudes[i, j]
                combined.append((2.0 * this - amplitudes[j, i]).astype(jnp.bfloat16))
                rounded.append(this.astype(jnp.bfloat16))
                turned.append((pltpu.roll(this, BAND, 1) * sign).astype(jnp.bfloat16))
        left = jnp.concatenate(combined, axis=1)
        spare = jnp.zeros((tiles * LANES - virtuals, left.shape[1]), jnp.bfloat16)
        for part, pieces_of in enumerate((rounded, turned)):
            right = jnp.concatenate([jnp.concatenate(pieces_of, axis=1), spare], axis=0)
            total[slot, part] += lax.dot_general(
                left, right, (((1,), (1,)), ((), ())), preferred_element_type=jnp.float32
            )

    def near_step(step):
        for piece in range(per_step):
            near_copy(step * per_step + piece, False).wait_recv()
        shape_mate(0, step)

    total[...] = jnp.zeros_like(total)
    early = steps - (BAND // PIECE - 1)
    lax.fori_loop(0, early, shape_own, 0)

    def main_step(piece, carry):
        forward(piece)

        @pl.when(piece == 1)
        def _():
            energy_far().wait_recv()

            @pl.when(odd == 1)
            def _():
                energy_near(True).start()

        even_piece = lax.rem(piece, 2) == 0

        @pl.when(lax.rem(piece, per_step) == per_step - 1)
        def _():
            shape_mate(1, piece // per_step)

        @pl.when(jnp.logical_and(even_piece, piece >= 4))
        def _():
            near_step(piece // 2 - 2)

        @pl.when(piece < steps - early)
        def _():
            shape_own(early + piece, 0)

        @pl.when(piece == steps - early)
        def _():
            shape_energies()

        phase = lax.rem(piece, BAND // PIECE)
        ready = jnp.logical_and(piece >= BAND // PIECE, jnp.logical_or(phase == 0, phase == 3))

        @pl.when(ready)
        def _():
            add_band(jnp.where(phase == 0, 1, 0), piece // (BAND // PIECE) - 1)

        return carry

    lax.fori_loop(0, pieces, main_step, 0)

    def swap_copy(slot):
        return pltpu.make_async_remote_copy(
            src_ref=outgoing.at[slot], dst_ref=incoming.at[slot],
            send_sem=swap_send.at[slot], recv_sem=swap_recv.at[slot],
            device_id=(me, other), device_id_type=mesh_id,
        )

    def half_rows(which):
        return pl.ds(pl.multiple_of(which * half, half), half)

    def places():
        for part in range(2):
            for tile in range(tiles):
                yield part, pl.ds(tile * LANES, LANES), pl.ds(tile * 2 + part, half, stride)

    def swap_start(slot):
        for part, lanes, spots in places():
            outgoing[slot, spots, :] = total[slot, part, half_rows(other), lanes]
        swap_copy(slot).start()

    near_step(steps - 2)
    add_band(1, bands - 1)
    swap_start(1)
    for momentum in range(2):
        for part, lanes, spots in places():
            known = total[1, part, half_rows(core), lanes]
            out_ref[momentum, spots, :] = jnp.where(chosen[1] == momentum, known, 0.0)
    near_step(steps - 1)
    add_band(0, bands - 1)
    swap_start(0)

    def drain(piece, carry):
        far_copy(piece).wait_send()
        near_copy(piece, False).wait_send()
        return carry

    lax.fori_loop(0, pieces, drain, 0)
    energy_far().wait_send()
    energy_near(False).wait_send()
    swap_copy(1).wait()
    for momentum in range(2):
        out_ref[momentum] += jnp.where(chosen[1] == momentum, 0.0, incoming[1])
        for part, lanes, spots in places():
            known = total[0, part, half_rows(core), lanes]
            out_ref[momentum, spots, :] += jnp.where(chosen[0] == momentum, known, 0.0)
    swap_copy(0).wait()
    for momentum in range(2):
        out_ref[momentum] += jnp.where(chosen[0] == momentum, 0.0, incoming[0])


def fused(factors, occupied_energy, virtual_energy, conserve, pair_lists):
    momenta, orbitals, virtuals, parts, auxiliary = factors.shape
    ring = lax.axis_size("ka")
    pieces = virtuals // PIECE
    bands = virtuals // BAND
    half = virtuals // 2
    tiles = pl.cdiv(virtuals, LANES)
    packed = (half * 2 * tiles, LANES)
    dma = pltpu.SemaphoreType.DMA
    density = pl.pallas_call(
        functools.partial(fused_kernel, ring, virtuals, auxiliary),
        out_shape=pltpu.VMEM((momenta, *packed), jnp.float32),
        in_specs=[
            pl.BlockSpec(memory_space=pltpu.HBM),
            pl.BlockSpec(memory_space=pltpu.HBM),
            pl.BlockSpec(memory_space=pltpu.HBM),
            pl.BlockSpec(memory_space=pltpu.HBM),
        ],
        out_specs=pl.BlockSpec(memory_space=pltpu.VMEM),
        scratch_shapes=[
            pltpu.SMEM(conserve.shape, conserve.dtype),
            pltpu.SMEM(occupied_energy.shape, occupied_energy.dtype),
            pltpu.VMEM(virtual_energy.shape, virtual_energy.dtype),
            pltpu.VMEM((momenta, orbitals, virtuals, parts, auxiliary), jnp.bfloat16),
            pltpu.VMEM((2, orbitals, virtuals, parts, auxiliary), jnp.bfloat16),
            pltpu.VMEM((momenta, orbitals * virtuals, parts * auxiliary), jnp.bfloat16),
            pltpu.VMEM((2, bands, orbitals * 2 * BAND, parts * auxiliary), jnp.bfloat16),
            pltpu.VMEM((2, momenta, virtuals), jnp.bfloat16),
            pltpu.VMEM((momenta, virtuals, LANES), jnp.float32),
            pltpu.VMEM((2, bands, 3, virtuals, LANES), jnp.float32),
            pltpu.VMEM((orbitals * virtuals, orbitals * 2 * BAND), jnp.float32),
            pltpu.VMEM((2, 2, virtuals, tiles * LANES), jnp.float32),
            pltpu.VMEM((2, *packed), jnp.float32),
            pltpu.VMEM((2, *packed), jnp.float32),
            dma((3,)), dma((2,)),
            dma((pieces,)), dma((pieces,)), dma((pieces,)), dma((pieces,)),
            dma((2,)), dma((2,)), dma((2,)), dma((2,)),
        ],
        compiler_params=pltpu.CompilerParams(
            collective_id=0, has_side_effects=True, vmem_limit_bytes=54 * 1024 * 1024
        ),
        name="density",
    )(conserve, occupied_energy, virtual_energy, factors)
    split = density.reshape(momenta, half, tiles, 2, LANES).transpose(0, 1, 3, 2, 4)
    return split.reshape(momenta, half, 2, tiles * LANES)[..., :virtuals]


def local(factors, occupied_energy, virtual_energy, conserve, pair_lists):
    momenta, orbitals, virtuals, parts, auxiliary = factors.shape
    rounds, pairs = pair_lists.shape[:2]
    ring, holders = lax.axis_size("ka"), lax.axis_size("occ")
    whole_square = pairs * holders == orbitals * orbitals
    fits = momenta == 2 and orbitals == 2 and holders == 2 and rounds == 2
    even = ring % 2 == 0 and ring > 4 and auxiliary % LANES == 0
    banded = virtuals % BAND == 0 and virtuals >= 2 * BAND
    chosen = fused if whole_square and fits and even and banded else general
    return chosen(factors, occupied_energy, virtual_energy, conserve, pair_lists)


def solution(mesh):
    in_specs = (
        P("ka", None, None, None, None),
        P(),
        P("ka", None),
        P("ka", None),
        P(None, "occ", None),
    )
    out_specs = P("ka", "occ", None, None)
    return jax.shard_map(local, mesh=mesh, in_specs=in_specs, out_specs=out_specs, check_vma=False)
```

```python
import functools

import jax
import jax.numpy as jnp
from jax import lax
from jax.experimental import pallas as pl
from jax.experimental.pallas import tpu as pltpu
from jax.sharding import PartitionSpec as P

LANES = 128
BAND = 64
STEP = 16
PIECE = 8
LAST = 3


def from_behind(array, axis, by):
    size = lax.axis_size(axis)
    return lax.ppermute(array, axis, [(i, (i + by) % size) for i in range(size)])


def build_mates(received, auxiliary):
    real_part = received[..., :auxiliary]
    imaginary = received[..., auxiliary:]
    turned = jnp.concatenate([-imaginary, real_part], axis=-1)
    return jnp.concatenate([received, turned], axis=-2)


def amplitude(left_rows, mate_rows, energy_left, energy_right, occupied_sum):
    values = lax.dot_general(
        left_rows, mate_rows, (((1,), (1,)), ((), ())), preferred_element_type=jnp.float32
    )
    denominator = energy_left[:, None] + energy_right[None, :] - occupied_sum
    return values / jnp.concatenate([denominator, denominator], axis=1)


def density_term(amplitudes, swapped):
    virtuals = amplitudes.shape[0]
    combined = (2.0 * amplitudes - swapped).astype(jnp.bfloat16)
    rounded = amplitudes.astype(jnp.bfloat16)
    turned = jnp.concatenate([-rounded[:, virtuals:], rounded[:, :virtuals]], axis=1)
    stacked = jnp.concatenate([rounded, turned], axis=0)
    return lax.dot_general(
        combined, stacked, (((1,), (1,)), ((), ())), preferred_element_type=jnp.float32
    )


def pair_term(own_block, mate_block, energy_left, energy_right, occupied_energy, pair_row):
    leading = pair_row[0]
    trailing = pair_row[1]
    occupied_sum = occupied_energy[leading] + occupied_energy[trailing]
    amplitudes = amplitude(
        own_block[leading], mate_block[trailing], energy_left, energy_right, occupied_sum
    )
    swapped = amplitude(
        own_block[trailing], mate_block[leading], energy_left, energy_right, occupied_sum
    )
    return density_term(amplitudes, swapped)


def general(factors, occupied_energy, virtual_energy, conserve, pair_lists):
    momenta = factors.shape[0]
    orbitals = factors.shape[1]
    virtuals = factors.shape[2]
    auxiliary = factors.shape[4]
    own = factors.reshape(momenta, orbitals, virtuals, 2 * auxiliary)
    energy_own = virtual_energy.astype(jnp.float32)
    density = jnp.zeros((momenta, virtuals, 2 * virtuals), jnp.float32)
    for round_index in range(conserve.shape[1]):
        portion = orbitals // lax.axis_size("occ")
        portion_block = lax.dynamic_slice_in_dim(
            factors, lax.axis_index("occ") * portion, portion, 1
        )
        shifted, energy_mate = from_behind((portion_block, virtual_energy), "ka", round_index + 1)
        received = lax.all_gather(shifted, "occ", axis=1, tiled=True)
        mates = build_mates(received.reshape(momenta, orbitals, virtuals, 2 * auxiliary), auxiliary)
        energy_mate = energy_mate.astype(jnp.float32)
        for local_index in range(momenta):
            chosen = (momenta - conserve[local_index, round_index] % momenta) % momenta
            mate_block = lax.dynamic_index_in_dim(mates, chosen, 0, keepdims=False)
            energy_right = lax.dynamic_index_in_dim(energy_mate, chosen, 0, keepdims=False)
            own_block = own[local_index]
            energy_left = energy_own[local_index]

            def add_pair(partial_sum, pair_row):
                term = pair_term(
                    own_block, mate_block, energy_left, energy_right, occupied_energy, pair_row
                )
                return (partial_sum + term, None)

            running, ignored = lax.scan(add_pair, density[local_index], pair_lists[round_index])
            density = density.at[local_index].set(running)
    shaped = density.reshape(momenta, virtuals, 2, virtuals)
    return lax.psum_scatter(shaped, "occ", scatter_dimension=1, tiled=True)


def fused_kernel(
    ring, virtuals, auxiliary,
    conserve_hbm, occupied_hbm, energy_hbm, factors_ref, out_ref,
    conserve_ref, occupied_ref, energy_ref, own_raw, mate_raw, side, own, mate, energy_in, energy_left, inverse, products, total, outgoing, incoming,
    small_sem, own_sem, far_send, far_recv, near_send, near_recv,
    energy_send, energy_recv, swap_send, swap_recv, side_send, side_recv,
):
    mesh_id = pl.DeviceIdType.MESH
    me = lax.axis_index("ka")
    core = lax.axis_index("occ")
    other = 1 - core
    odd = lax.rem(me, 2)
    half = virtuals // 2
    pieces = virtuals // PIECE
    steps = virtuals // STEP
    bands = virtuals // BAND
    per_step = STEP // PIECE
    per_band = BAND // STEP
    tiles = pl.cdiv(virtuals, LANES)
    stride = 2 * tiles

    def at(step):
        return lax.rem(me + step + ring, ring)

    near = at(1 - 2 * odd)

    def own_copy(momentum, index):
        return pltpu.make_async_copy(
            factors_ref.at[momentum], own_raw.at[momentum], own_sem.at[index]
        )

    def small_copies():
        return (
            pltpu.make_async_copy(conserve_hbm, conserve_ref, small_sem.at[0]),
            pltpu.make_async_copy(occupied_hbm, occupied_ref, small_sem.at[1]),
            pltpu.make_async_copy(energy_hbm, energy_ref, small_sem.at[2]),
        )

    barrier = pltpu.get_barrier_semaphore()
    for place in ((at(-2), core), (near, core), (me, other)):
        pl.semaphore_signal(barrier, inc=1, device_id=place, device_id_type=mesh_id)
    for listener, speaker in ((0, ring - 4), (ring - 4, ring - 1)):
        @pl.when(me == listener)
        def _():
            pl.semaphore_signal(
                barrier, inc=1, device_id=(speaker, core), device_id_type=mesh_id
            )

    own_copy(core, 0).start()
    for copy in small_copies():
        copy.start()
    own_copy(other, 1).start()

    def piece_rows(piece):
        return pl.ds(pl.multiple_of(piece * PIECE, PIECE), PIECE)

    def step_rows(step):
        return pl.ds(pl.multiple_of(step * STEP, STEP), STEP)

    def far_copy(piece):
        return pltpu.make_async_remote_copy(
            src_ref=factors_ref.at[core, :, piece_rows(piece)],
            dst_ref=mate_raw.at[1, :, piece_rows(piece)],
            send_sem=far_send.at[0], recv_sem=far_recv.at[piece],
            device_id=(at(2), core), device_id_type=mesh_id,
        )

    def near_copy(piece, relay):
        source = mate_raw.at[1] if relay else factors_ref.at[core]
        return pltpu.make_async_remote_copy(
            src_ref=source.at[:, piece_rows(piece)],
            dst_ref=mate_raw.at[0, :, piece_rows(piece)],
            send_sem=near_send.at[0], recv_sem=near_recv.at[piece // per_step],
            device_id=(near, core), device_id_type=mesh_id,
        )

    def near_arrival(step):
        rows = mate_raw.at[0, :, step_rows(step)]
        return pltpu.make_async_copy(rows, rows, near_recv.at[step])

    def lend_copy(slot):
        piece = pieces - LAST + slot
        return pltpu.make_async_remote_copy(
            src_ref=factors_ref.at[core, :, piece_rows(piece)], dst_ref=side.at[slot],
            send_sem=side_send.at[0], recv_sem=side_recv.at[slot],
            device_id=(ring - 4, core), device_id_type=mesh_id,
        )

    def carry_copy(slot):
        piece = pieces - LAST + slot
        return pltpu.make_async_remote_copy(
            src_ref=side.at[slot], dst_ref=mate_raw.at[0, :, piece_rows(piece)],
            send_sem=side_send.at[0], recv_sem=near_recv.at[piece // per_step],
            device_id=(0, core), device_id_type=mesh_id,
        )

    def energy_far():
        return pltpu.make_async_remote_copy(
            src_ref=energy_ref, dst_ref=energy_in.at[1],
            send_sem=energy_send.at[1], recv_sem=energy_recv.at[1],
            device_id=(at(2), core), device_id_type=mesh_id,
        )

    def energy_near(relay):
        return pltpu.make_async_remote_copy(
            src_ref=energy_in.at[1] if relay else energy_ref, dst_ref=energy_in.at[0],
            send_sem=energy_send.at[0], recv_sem=energy_recv.at[0],
            device_id=(near, core), device_id_type=mesh_id,
        )

    greeters = jnp.where(jnp.logical_or(me == ring - 1, me == ring - 4), 4, 3)
    pl.semaphore_wait(barrier, greeters)

    @pl.when(me == ring - 1)
    def _():
        for slot in range(LAST):
            lend_copy(slot).start()

    def send_piece(piece, carry):
        far_copy(piece).start()

        @pl.when(odd == 0)
        def _():
            near_copy(piece, False).start()

        return carry

    lax.fori_loop(0, 2, send_piece, 0)
    for copy in small_copies():
        copy.wait()
    energy_far().start()

    @pl.when(odd == 0)
    def _():
        energy_near(False).start()

    lax.fori_loop(2, pieces, send_piece, 0)

    chosen = []
    for slot in range(2):
        mirror = lax.rem(2 - lax.rem(conserve_ref[0, slot], 2), 2)
        chosen.append(jnp.where(mirror == core, 0, 1))

    own_copy(core, 0).wait()
    own_copy(other, 1).wait()

    def forward(piece):
        far_copy(piece).wait_recv()

        @pl.when(jnp.logical_and(odd == 1, jnp.logical_or(me != 1, piece < pieces - LAST)))
        def _():
            near_copy(piece, True).start()

    def shape_own(step, carry):
        for momentum in range(2):
            for orbital in range(2):
                row = pl.ds(pl.multiple_of(orbital * virtuals + step * STEP, STEP), STEP)
                for part in range(2):
                    own[momentum, row, pl.ds(part * auxiliary, auxiliary)] = own_raw[
                        momentum, orbital, step_rows(step), part, :
                    ]
        return carry

    def shape_mate(slot, step):
        band = step // per_band
        for orbital in range(2):
            real = mate_raw[slot, orbital, step_rows(step), 0, :]
            imaginary = mate_raw[slot, orbital, step_rows(step), 1, :]
            first = orbital * 2 * BAND + lax.rem(step, per_band) * STEP
            plain = pl.ds(pl.multiple_of(first, STEP), STEP)
            turned = pl.ds(pl.multiple_of(first + BAND, STEP), STEP)
            mate[slot, band, plain, pl.ds(0, auxiliary)] = real
            mate[slot, band, plain, pl.ds(auxiliary, auxiliary)] = imaginary
            mate[slot, band, turned, pl.ds(0, auxiliary)] = -imaginary
            mate[slot, band, turned, pl.ds(auxiliary, auxiliary)] = real

    def shape_energies():
        sums = [occupied_ref[0] + occupied_ref[0], occupied_ref[0] + occupied_ref[1]]
        sums.append(occupied_ref[1] + occupied_ref[1])
        diagonal = lax.broadcasted_iota(
            jnp.int32, (virtuals, virtuals), 0
        ) == lax.broadcasted_iota(jnp.int32, (virtuals, virtuals), 1)
        mine = energy_ref[...].astype(jnp.float32)
        for momentum in range(2):
            spread = jnp.where(diagonal, mine[momentum : momentum + 1, :], 0.0)
            column = jnp.sum(spread, axis=1, keepdims=True)
            energy_left[momentum] = jnp.broadcast_to(column, (virtuals, LANES))
        energy_near(False).wait_recv()
        for slot in range(2):
            theirs = energy_in[slot].astype(jnp.float32)
            theirs = jnp.where(core == 0, theirs[0:1, :], theirs[1:2, :])
            for band in range(bands):
                part = theirs[:, band * BAND : (band + 1) * BAND]
                row = jnp.concatenate([part, part], axis=1)
                base = energy_left[chosen[slot]] + row
                for kind in range(3):
                    inverse[slot, band, kind] = 1.0 / (base - sums[kind])

    sign = jnp.where(lax.broadcasted_iota(jnp.int32, (virtuals, LANES), 1) < BAND, -1.0, 1.0)

    def add_band(slot, band):
        momentum = jnp.where(slot == 1, chosen[1], chosen[0])
        products[...] = lax.dot_general(
            own[momentum], mate[slot, band], (((1,), (1,)), ((), ())),
            preferred_element_type=jnp.float32,
        )
        amplitudes = {}
        for i in range(2):
            for j in range(2):
                value = products[i * virtuals : (i + 1) * virtuals, j * LANES : (j + 1) * LANES]
                amplitudes[i, j] = value * inverse[slot, band, i + j]
        combined, rounded, turned = [], [], []
        for i in range(2):
            for j in range(2):
                this = amplitudes[i, j]
                combined.append((2.0 * this - amplitudes[j, i]).astype(jnp.bfloat16))
                rounded.append(this.astype(jnp.bfloat16))
                turned.append((pltpu.roll(this, BAND, 1) * sign).astype(jnp.bfloat16))
        left = jnp.concatenate(combined, axis=1)
        spare = jnp.zeros((tiles * LANES - virtuals, left.shape[1]), jnp.bfloat16)
        for part, pieces_of in enumerate((rounded, turned)):
            right = jnp.concatenate([jnp.concatenate(pieces_of, axis=1), spare], axis=0)
            total[slot, part] += lax.dot_general(
                left, right, (((1,), (1,)), ((), ())), preferred_element_type=jnp.float32
            )

    def near_step(step):
        near_arrival(step).wait()
        shape_mate(0, step)

    total[...] = jnp.zeros_like(total)
    early = steps - (BAND // PIECE - 1)
    lax.fori_loop(0, early, shape_own, 0)

    def main_step(piece, carry):
        forward(piece)

        for slot in range(LAST):
            @pl.when(jnp.logical_and(me == ring - 4, piece == slot + 8))
            def _():
                lend_copy(slot).wait_recv()
                carry_copy(slot).start()

        @pl.when(jnp.logical_and(me == 0, piece == pieces - 3))
        def _():
            near_step(steps - 1)

        @pl.when(piece == 1)
        def _():
            energy_far().wait_recv()

            @pl.when(odd == 1)
            def _():
                energy_near(True).start()

        even_piece = lax.rem(piece, 2) == 0

        @pl.when(lax.rem(piece, per_step) == per_step - 1)
        def _():
            shape_mate(1, piece // per_step)

        @pl.when(jnp.logical_and(even_piece, piece >= 4))
        def _():
            near_step(piece // 2 - 2)

        @pl.when(piece < steps - early)
        def _():
            shape_own(early + piece, 0)

        @pl.when(piece == steps - early)
        def _():
            shape_energies()

        phase = lax.rem(piece, BAND // PIECE)
        ready = jnp.logical_and(piece >= BAND // PIECE, jnp.logical_or(phase == 0, phase == 3))

        @pl.when(ready)
        def _():
            add_band(jnp.where(phase == 0, 1, 0), piece // (BAND // PIECE) - 1)

        return carry

    lax.fori_loop(0, pieces - per_step, main_step, 0)

    def swap_copy(slot):
        return pltpu.make_async_remote_copy(
            src_ref=outgoing.at[slot], dst_ref=incoming.at[slot],
            send_sem=swap_send.at[slot], recv_sem=swap_recv.at[slot],
            device_id=(me, other), device_id_type=mesh_id,
        )

    def half_rows(which):
        return pl.ds(pl.multiple_of(which * half, half), half)

    def places():
        for part in range(2):
            for tile in range(tiles):
                yield part, pl.ds(tile * LANES, LANES), pl.ds(tile * 2 + part, half, stride)

    def swap_start(slot):
        for part, lanes, spots in places():
            outgoing[slot, spots, :] = total[slot, part, half_rows(other), lanes]
        swap_copy(slot).start()

    def sent(done, semaphore):
        pltpu.make_async_copy(done, done, semaphore).wait()

    def finish(first, second, before_first, before_second):
        before_first()
        add_band(first, bands - 1)
        swap_start(first)
        for momentum in range(2):
            for part, lanes, spots in places():
                known = total[first, part, half_rows(core), lanes]
                out_ref[momentum, spots, :] = jnp.where(chosen[first] == momentum, known, 0.0)
        before_second()
        add_band(second, bands - 1)
        swap_start(second)
        swap_copy(first).wait()
        for momentum in range(2):
            out_ref[momentum] += jnp.where(chosen[first] == momentum, 0.0, incoming[first])
            for part, lanes, spots in places():
                known = total[second, part, half_rows(core), lanes]
                out_ref[momentum, spots, :] += jnp.where(chosen[second] == momentum, known, 0.0)
        sent(own_raw.at[core], far_send.at[0])
        swap_copy(second).wait()
        for momentum in range(2):
            out_ref[momentum] += jnp.where(chosen[second] == momentum, 0.0, incoming[second])

    near_first = jnp.logical_or(me == 0, me == ring - 4)

    @pl.when(near_first)
    def _():
        def near_rest():
            near_step(steps - 3)
            near_step(steps - 2)

            @pl.when(me != 0)
            def _():
                near_step(steps - 1)

        def far_rest():
            for piece in range(pieces - per_step, pieces):
                forward(piece)
            shape_mate(1, steps - 1)

        finish(0, 1, near_rest, far_rest)

    @pl.when(jnp.logical_not(near_first))
    def _():
        def far_rest():
            forward(pieces - 2)
            near_step(steps - 3)
            forward(pieces - 1)
            shape_mate(1, steps - 1)
            near_step(steps - 2)

        finish(1, 0, far_rest, lambda: near_step(steps - 1))

    energy_far().wait_send()
    energy_near(False).wait_send()

    @pl.when(me == 1)
    def _():
        sent(own_raw.at[core, :, pl.ds(0, virtuals - LAST * PIECE)], near_send.at[0])

    @pl.when(me != 1)
    def _():
        sent(own_raw.at[core], near_send.at[0])

    @pl.when(jnp.logical_or(me == ring - 1, me == ring - 4))
    def _():
        sent(side, side_send.at[0])


def fused(factors, occupied_energy, virtual_energy, conserve, pair_lists):
    momenta, orbitals, virtuals, parts, auxiliary = factors.shape
    ring = lax.axis_size("ka")
    pieces = virtuals // PIECE
    bands = virtuals // BAND
    half = virtuals // 2
    tiles = pl.cdiv(virtuals, LANES)
    packed = (half * 2 * tiles, LANES)
    dma = pltpu.SemaphoreType.DMA
    density = pl.pallas_call(
        functools.partial(fused_kernel, ring, virtuals, auxiliary),
        out_shape=pltpu.VMEM((momenta, *packed), jnp.float32),
        in_specs=[
            pl.BlockSpec(memory_space=pltpu.HBM),
            pl.BlockSpec(memory_space=pltpu.HBM),
            pl.BlockSpec(memory_space=pltpu.HBM),
            pl.BlockSpec(memory_space=pltpu.HBM),
        ],
        out_specs=pl.BlockSpec(memory_space=pltpu.VMEM),
        scratch_shapes=[
            pltpu.SMEM(conserve.shape, conserve.dtype),
            pltpu.SMEM(occupied_energy.shape, occupied_energy.dtype),
            pltpu.VMEM(virtual_energy.shape, virtual_energy.dtype),
            pltpu.VMEM((momenta, orbitals, virtuals, parts, auxiliary), jnp.bfloat16),
            pltpu.VMEM((2, orbitals, virtuals, parts, auxiliary), jnp.bfloat16),
            pltpu.VMEM((LAST, orbitals, PIECE, parts, auxiliary), jnp.bfloat16),
            pltpu.VMEM((momenta, orbitals * virtuals, parts * auxiliary), jnp.bfloat16),
            pltpu.VMEM((2, bands, orbitals * 2 * BAND, parts * auxiliary), jnp.bfloat16),
            pltpu.VMEM((2, momenta, virtuals), jnp.bfloat16),
            pltpu.VMEM((momenta, virtuals, LANES), jnp.float32),
            pltpu.VMEM((2, bands, 3, virtuals, LANES), jnp.float32),
            pltpu.VMEM((orbitals * virtuals, orbitals * 2 * BAND), jnp.float32),
            pltpu.VMEM((2, 2, virtuals, tiles * LANES), jnp.float32),
            pltpu.VMEM((2, *packed), jnp.float32),
            pltpu.VMEM((2, *packed), jnp.float32),
            dma((3,)), dma((2,)),
            dma((1,)), dma((pieces,)), dma((1,)), dma((virtuals // STEP,)),
            dma((2,)), dma((2,)), dma((2,)), dma((2,)),
            dma((1,)), dma((LAST,)),
        ],
        compiler_params=pltpu.CompilerParams(
            collective_id=0, has_side_effects=True, vmem_limit_bytes=54 * 1024 * 1024
        ),
        name="density",
    )(conserve, occupied_energy, virtual_energy, factors)
    split = density.reshape(momenta, half, tiles, 2, LANES).transpose(0, 1, 3, 2, 4)
    return split.reshape(momenta, half, 2, tiles * LANES)[..., :virtuals]


def local(factors, occupied_energy, virtual_energy, conserve, pair_lists):
    momenta, orbitals, virtuals, parts, auxiliary = factors.shape
    rounds, pairs = pair_lists.shape[:2]
    ring, holders = lax.axis_size("ka"), lax.axis_size("occ")
    whole_square = pairs * holders == orbitals * orbitals
    fits = momenta == 2 and orbitals == 2 and holders == 2 and rounds == 2
    even = ring % 2 == 0 and ring > 6 and auxiliary % LANES == 0
    banded = virtuals % BAND == 0 and virtuals >= 2 * BAND
    chosen = fused if whole_square and fits and even and banded else general
    return chosen(factors, occupied_energy, virtual_energy, conserve, pair_lists)


def solution(mesh):
    in_specs = (
        P("ka", None, None, None, None),
        P(),
        P("ka", None),
        P("ka", None),
        P(None, "occ", None),
    )
    out_specs = P("ka", "occ", None, None)
    return jax.shard_map(local, mesh=mesh, in_specs=in_specs, out_specs=out_specs, check_vma=False)
```

```python
import functools

import jax
import jax.numpy as jnp
from jax import lax
from jax.experimental import pallas as pl
from jax.experimental.pallas import tpu as pltpu
from jax.sharding import PartitionSpec as P

LANES = 128
BAND = 64
STEP = 16
PIECE = 8
LAST = 4
MOST = 4


def from_behind(array, axis, by):
    size = lax.axis_size(axis)
    return lax.ppermute(array, axis, [(i, (i + by) % size) for i in range(size)])


def build_mates(received, auxiliary):
    real_part = received[..., :auxiliary]
    imaginary = received[..., auxiliary:]
    turned = jnp.concatenate([-imaginary, real_part], axis=-1)
    return jnp.concatenate([received, turned], axis=-2)


def amplitude(left_rows, mate_rows, energy_left, energy_right, occupied_sum):
    values = lax.dot_general(
        left_rows, mate_rows, (((1,), (1,)), ((), ())), preferred_element_type=jnp.float32
    )
    denominator = energy_left[:, None] + energy_right[None, :] - occupied_sum
    return values / jnp.concatenate([denominator, denominator], axis=1)


def density_term(amplitudes, swapped):
    virtuals = amplitudes.shape[0]
    combined = (2.0 * amplitudes - swapped).astype(jnp.bfloat16)
    rounded = amplitudes.astype(jnp.bfloat16)
    turned = jnp.concatenate([-rounded[:, virtuals:], rounded[:, :virtuals]], axis=1)
    stacked = jnp.concatenate([rounded, turned], axis=0)
    return lax.dot_general(
        combined, stacked, (((1,), (1,)), ((), ())), preferred_element_type=jnp.float32
    )


def pair_term(own_block, mate_block, energy_left, energy_right, occupied_energy, pair_row):
    leading = pair_row[0]
    trailing = pair_row[1]
    occupied_sum = occupied_energy[leading] + occupied_energy[trailing]
    amplitudes = amplitude(
        own_block[leading], mate_block[trailing], energy_left, energy_right, occupied_sum
    )
    swapped = amplitude(
        own_block[trailing], mate_block[leading], energy_left, energy_right, occupied_sum
    )
    return density_term(amplitudes, swapped)


def general(factors, occupied_energy, virtual_energy, conserve, pair_lists):
    momenta = factors.shape[0]
    orbitals = factors.shape[1]
    virtuals = factors.shape[2]
    auxiliary = factors.shape[4]
    own = factors.reshape(momenta, orbitals, virtuals, 2 * auxiliary)
    energy_own = virtual_energy.astype(jnp.float32)
    density = jnp.zeros((momenta, virtuals, 2 * virtuals), jnp.float32)
    for round_index in range(conserve.shape[1]):
        portion = orbitals // lax.axis_size("occ")
        portion_block = lax.dynamic_slice_in_dim(
            factors, lax.axis_index("occ") * portion, portion, 1
        )
        shifted, energy_mate = from_behind((portion_block, virtual_energy), "ka", round_index + 1)
        received = lax.all_gather(shifted, "occ", axis=1, tiled=True)
        mates = build_mates(received.reshape(momenta, orbitals, virtuals, 2 * auxiliary), auxiliary)
        energy_mate = energy_mate.astype(jnp.float32)
        for local_index in range(momenta):
            chosen = (momenta - conserve[local_index, round_index] % momenta) % momenta
            mate_block = lax.dynamic_index_in_dim(mates, chosen, 0, keepdims=False)
            energy_right = lax.dynamic_index_in_dim(energy_mate, chosen, 0, keepdims=False)
            own_block = own[local_index]
            energy_left = energy_own[local_index]

            def add_pair(partial_sum, pair_row):
                term = pair_term(
                    own_block, mate_block, energy_left, energy_right, occupied_energy, pair_row
                )
                return (partial_sum + term, None)

            running, ignored = lax.scan(add_pair, density[local_index], pair_lists[round_index])
            density = density.at[local_index].set(running)
    shaped = density.reshape(momenta, virtuals, 2, virtuals)
    return lax.psum_scatter(shaped, "occ", scatter_dimension=1, tiled=True)


def fused_kernel(
    ring, virtuals, auxiliary,
    conserve_hbm, occupied_hbm, energy_hbm, factors_ref, out_ref,
    conserve_ref, occupied_ref, energy_ref, own_raw, mate_raw, side, loan, own, mate, energy_in, energy_left, inverse, products, total, outgoing, incoming,
    small_sem, own_sem, far_send, far_recv, near_send, near_recv,
    energy_send, energy_recv, swap_send, swap_recv, side_send, side_recv, loan_send, loan_recv,
):
    mesh_id = pl.DeviceIdType.MESH
    me = lax.axis_index("ka")
    core = lax.axis_index("occ")
    other = 1 - core
    odd = lax.rem(me, 2)
    half = virtuals // 2
    pieces = virtuals // PIECE
    steps = virtuals // STEP
    bands = virtuals // BAND
    per_step = STEP // PIECE
    per_band = BAND // STEP
    tiles = pl.cdiv(virtuals, LANES)
    stride = 2 * tiles

    def at(step):
        return lax.rem(me + step + ring, ring)

    near = at(1 - 2 * odd)
    lender = jnp.logical_and(lax.rem(me, 4) == 2, me != ring - 2)
    carrier = jnp.logical_and(lax.rem(me, 4) == 0, me != ring - 4)

    def lent(sender):
        return jnp.minimum(2 + sender // 4, MOST)

    def keeps(piece):
        return jnp.logical_or(jnp.logical_not(lender), piece < pieces - lent(me))

    def own_copy(momentum, index):
        return pltpu.make_async_copy(
            factors_ref.at[momentum], own_raw.at[momentum], own_sem.at[index]
        )

    def small_copies():
        return (
            pltpu.make_async_copy(conserve_hbm, conserve_ref, small_sem.at[0]),
            pltpu.make_async_copy(occupied_hbm, occupied_ref, small_sem.at[1]),
            pltpu.make_async_copy(energy_hbm, energy_ref, small_sem.at[2]),
        )

    barrier = pltpu.get_barrier_semaphore()
    for place in ((at(-2), core), (near, core), (me, other)):
        pl.semaphore_signal(barrier, inc=1, device_id=place, device_id_type=mesh_id)
    for listener, speaker in ((0, ring - 4), (ring - 4, ring - 1)):
        @pl.when(me == listener)
        def _():
            pl.semaphore_signal(
                barrier, inc=1, device_id=(speaker, core), device_id_type=mesh_id
            )

    @pl.when(carrier)
    def _():
        pl.semaphore_signal(barrier, inc=1, device_id=(at(2), core), device_id_type=mesh_id)

    @pl.when(jnp.logical_and(lax.rem(me, 4) == 0, me != 0))
    def _():
        pl.semaphore_signal(barrier, inc=1, device_id=(at(-4), core), device_id_type=mesh_id)

    own_copy(core, 0).start()
    for copy in small_copies():
        copy.start()
    own_copy(other, 1).start()

    def piece_rows(piece):
        return pl.ds(pl.multiple_of(piece * PIECE, PIECE), PIECE)

    def step_rows(step):
        return pl.ds(pl.multiple_of(step * STEP, STEP), STEP)

    def far_copy(piece):
        return pltpu.make_async_remote_copy(
            src_ref=factors_ref.at[core, :, piece_rows(piece)],
            dst_ref=mate_raw.at[1, :, piece_rows(piece)],
            send_sem=far_send.at[0], recv_sem=far_recv.at[piece],
            device_id=(at(2), core), device_id_type=mesh_id,
        )

    def near_copy(piece, relay):
        source = mate_raw.at[1] if relay else factors_ref.at[core]
        return pltpu.make_async_remote_copy(
            src_ref=source.at[:, piece_rows(piece)],
            dst_ref=mate_raw.at[0, :, piece_rows(piece)],
            send_sem=near_send.at[0], recv_sem=near_recv.at[piece // per_step],
            device_id=(near, core), device_id_type=mesh_id,
        )

    def near_arrival(step):
        rows = mate_raw.at[0, :, step_rows(step)]
        return pltpu.make_async_copy(rows, rows, near_recv.at[step])

    def lend_copy(slot):
        piece = pieces - LAST + slot
        return pltpu.make_async_remote_copy(
            src_ref=factors_ref.at[core, :, piece_rows(piece)], dst_ref=side.at[slot],
            send_sem=side_send.at[0], recv_sem=side_recv.at[slot],
            device_id=(ring - 4, core), device_id_type=mesh_id,
        )

    def carry_copy(slot):
        piece = pieces - LAST + slot
        return pltpu.make_async_remote_copy(
            src_ref=side.at[slot], dst_ref=mate_raw.at[0, :, piece_rows(piece)],
            send_sem=side_send.at[0], recv_sem=near_recv.at[piece // per_step],
            device_id=(0, core), device_id_type=mesh_id,
        )

    def loan_copy(slot):
        return pltpu.make_async_remote_copy(
            src_ref=factors_ref.at[core, :, piece_rows(pieces - lent(me) + slot)],
            dst_ref=loan.at[slot],
            send_sem=far_send.at[0], recv_sem=loan_recv.at[slot],
            device_id=(at(-2), core), device_id_type=mesh_id,
        )

    def loan_carry(slot):
        piece = pieces - lent(me + 2) + slot
        return pltpu.make_async_remote_copy(
            src_ref=loan.at[slot], dst_ref=mate_raw.at[1, :, piece_rows(piece)],
            send_sem=loan_send.at[slot], recv_sem=far_recv.at[piece],
            device_id=(at(4), core), device_id_type=mesh_id,
        )

    def energy_far():
        return pltpu.make_async_remote_copy(
            src_ref=energy_ref, dst_ref=energy_in.at[1],
            send_sem=energy_send.at[1], recv_sem=energy_recv.at[1],
            device_id=(at(2), core), device_id_type=mesh_id,
        )

    def energy_near(relay):
        return pltpu.make_async_remote_copy(
            src_ref=energy_in.at[1] if relay else energy_ref, dst_ref=energy_in.at[0],
            send_sem=energy_send.at[0], recv_sem=energy_recv.at[0],
            device_id=(near, core), device_id_type=mesh_id,
        )

    extra = jnp.logical_or(jnp.logical_or(lender, carrier), me >= ring - 1)
    greeters = jnp.where(jnp.logical_or(extra, me == ring - 4), 4, 3)
    pl.semaphore_wait(barrier, greeters)

    @pl.when(me == ring - 1)
    def _():
        for slot in range(LAST):
            lend_copy(slot).start()

    for slot in range(MOST):
        @pl.when(jnp.logical_and(lender, slot < lent(me)))
        def _():
            loan_copy(slot).start()

    late = me == ring - 6

    def send_far(piece, carry):
        @pl.when(keeps(piece))
        def _():
            far_copy(piece).start()

        return carry

    def send_piece(piece, carry):
        @pl.when(jnp.logical_not(late))
        def _():
            send_far(piece, 0)

        @pl.when(odd == 0)
        def _():
            near_copy(piece, False).start()

        return carry

    lax.fori_loop(0, 2, send_piece, 0)
    for copy in small_copies():
        copy.wait()
    energy_far().start()

    @pl.when(odd == 0)
    def _():
        energy_near(False).start()

    lax.fori_loop(2, pieces, send_piece, 0)

    chosen = []
    for slot in range(2):
        mirror = lax.rem(2 - lax.rem(conserve_ref[0, slot], 2), 2)
        chosen.append(jnp.where(mirror == core, 0, 1))

    own_copy(core, 0).wait()
    own_copy(other, 1).wait()

    def forward(piece):
        far_copy(piece).wait_recv()

        @pl.when(jnp.logical_and(odd == 1, jnp.logical_or(me != 1, piece < pieces - LAST)))
        def _():
            near_copy(piece, True).start()

    def shape_own(step, carry):
        for momentum in range(2):
            for orbital in range(2):
                row = pl.ds(pl.multiple_of(orbital * virtuals + step * STEP, STEP), STEP)
                for part in range(2):
                    own[momentum, row, pl.ds(part * auxiliary, auxiliary)] = own_raw[
                        momentum, orbital, step_rows(step), part, :
                    ]
        return carry

    def shape_mate(slot, step):
        band = step // per_band
        for orbital in range(2):
            real = mate_raw[slot, orbital, step_rows(step), 0, :]
            imaginary = mate_raw[slot, orbital, step_rows(step), 1, :]
            first = orbital * 2 * BAND + lax.rem(step, per_band) * STEP
            plain = pl.ds(pl.multiple_of(first, STEP), STEP)
            turned = pl.ds(pl.multiple_of(first + BAND, STEP), STEP)
            mate[slot, band, plain, pl.ds(0, auxiliary)] = real
            mate[slot, band, plain, pl.ds(auxiliary, auxiliary)] = imaginary
            mate[slot, band, turned, pl.ds(0, auxiliary)] = -imaginary
            mate[slot, band, turned, pl.ds(auxiliary, auxiliary)] = real

    def shape_energies():
        sums = [occupied_ref[0] + occupied_ref[0], occupied_ref[0] + occupied_ref[1]]
        sums.append(occupied_ref[1] + occupied_ref[1])
        diagonal = lax.broadcasted_iota(
            jnp.int32, (virtuals, virtuals), 0
        ) == lax.broadcasted_iota(jnp.int32, (virtuals, virtuals), 1)
        mine = energy_ref[...].astype(jnp.float32)
        for momentum in range(2):
            spread = jnp.where(diagonal, mine[momentum : momentum + 1, :], 0.0)
            column = jnp.sum(spread, axis=1, keepdims=True)
            energy_left[momentum] = jnp.broadcast_to(column, (virtuals, LANES))
        energy_near(False).wait_recv()
        for slot in range(2):
            theirs = energy_in[slot].astype(jnp.float32)
            theirs = jnp.where(core == 0, theirs[0:1, :], theirs[1:2, :])
            for band in range(bands):
                part = theirs[:, band * BAND : (band + 1) * BAND]
                row = jnp.concatenate([part, part], axis=1)
                base = energy_left[chosen[slot]] + row
                for kind in range(3):
                    inverse[slot, band, kind] = 1.0 / (base - sums[kind])

    sign = jnp.where(lax.broadcasted_iota(jnp.int32, (virtuals, LANES), 1) < BAND, -1.0, 1.0)

    def add_band(slot, band):
        momentum = jnp.where(slot == 1, chosen[1], chosen[0])
        products[...] = lax.dot_general(
            own[momentum], mate[slot, band], (((1,), (1,)), ((), ())),
            preferred_element_type=jnp.float32,
        )
        amplitudes = {}
        for i in range(2):
            for j in range(2):
                value = products[i * virtuals : (i + 1) * virtuals, j * LANES : (j + 1) * LANES]
                amplitudes[i, j] = value * inverse[slot, band, i + j]
        combined, rounded, turned = [], [], []
        for i in range(2):
            for j in range(2):
                this = amplitudes[i, j]
                combined.append((2.0 * this - amplitudes[j, i]).astype(jnp.bfloat16))
                rounded.append(this.astype(jnp.bfloat16))
                turned.append((pltpu.roll(this, BAND, 1) * sign).astype(jnp.bfloat16))
        left = jnp.concatenate(combined, axis=1)
        spare = jnp.zeros((tiles * LANES - virtuals, left.shape[1]), jnp.bfloat16)
        for part, pieces_of in enumerate((rounded, turned)):
            right = jnp.concatenate([jnp.concatenate(pieces_of, axis=1), spare], axis=0)
            total[slot, part] += lax.dot_general(
                left, right, (((1,), (1,)), ((), ())), preferred_element_type=jnp.float32
            )

    def near_step(step):
        near_arrival(step).wait()
        shape_mate(0, step)

    total[...] = jnp.zeros_like(total)
    early = steps - (BAND // PIECE - 1)
    lax.fori_loop(0, early, shape_own, 0)

    @pl.when(late)
    def _():
        lax.fori_loop(0, pieces, send_far, 0)

    def main_step(piece, carry):
        @pl.when(jnp.logical_and(carrier, piece == jnp.where(me == 0, 6, pieces - 3)))
        def _():
            for slot in range(MOST):
                @pl.when(slot < lent(me + 2))
                def _():
                    loan_copy(slot).wait_recv()
                    loan_carry(slot).start()

        forward(piece)

        for slot in range(LAST):
            @pl.when(jnp.logical_and(me == ring - 4, piece == slot + 8))
            def _():
                lend_copy(slot).wait_recv()
                carry_copy(slot).start()

        for behind in (1, 2):
            @pl.when(jnp.logical_and(me == 0, piece == pieces - 1 - 2 * behind))
            def _():
                near_step(steps - behind)

        @pl.when(piece == 1)
        def _():
            energy_far().wait_recv()

            @pl.when(odd == 1)
            def _():
                energy_near(True).start()

        even_piece = lax.rem(piece, 2) == 0

        @pl.when(lax.rem(piece, per_step) == per_step - 1)
        def _():
            shape_mate(1, piece // per_step)

        @pl.when(jnp.logical_and(even_piece, piece >= 4))
        def _():
            near_step(piece // 2 - 2)

        @pl.when(piece < steps - early)
        def _():
            shape_own(early + piece, 0)

        @pl.when(piece == steps - early)
        def _():
            shape_energies()

        phase = lax.rem(piece, BAND // PIECE)
        ready = jnp.logical_and(piece >= BAND // PIECE, jnp.logical_or(phase == 0, phase == 3))

        @pl.when(ready)
        def _():
            add_band(jnp.where(phase == 0, 1, 0), piece // (BAND // PIECE) - 1)

        return carry

    lax.fori_loop(0, pieces - per_step, main_step, 0)

    def swap_copy(slot):
        return pltpu.make_async_remote_copy(
            src_ref=outgoing.at[slot], dst_ref=incoming.at[slot],
            send_sem=swap_send.at[slot], recv_sem=swap_recv.at[slot],
            device_id=(me, other), device_id_type=mesh_id,
        )

    def half_rows(which):
        return pl.ds(pl.multiple_of(which * half, half), half)

    def places():
        for part in range(2):
            for tile in range(tiles):
                yield part, pl.ds(tile * LANES, LANES), pl.ds(tile * 2 + part, half, stride)

    def swap_start(slot):
        for part, lanes, spots in places():
            outgoing[slot, spots, :] = total[slot, part, half_rows(other), lanes]
        swap_copy(slot).start()

    def sent(done, semaphore):
        pltpu.make_async_copy(done, done, semaphore).wait()

    def finish(first, second, before_first, before_second):
        before_first()
        add_band(first, bands - 1)
        swap_start(first)
        for momentum in range(2):
            for part, lanes, spots in places():
                known = total[first, part, half_rows(core), lanes]
                out_ref[momentum, spots, :] = jnp.where(chosen[first] == momentum, known, 0.0)
        before_second()
        add_band(second, bands - 1)
        swap_start(second)
        swap_copy(first).wait()
        for momentum in range(2):
            out_ref[momentum] += jnp.where(chosen[first] == momentum, 0.0, incoming[first])
            for part, lanes, spots in places():
                known = total[second, part, half_rows(core), lanes]
                out_ref[momentum, spots, :] += jnp.where(chosen[second] == momentum, known, 0.0)
        sent(own_raw.at[core], far_send.at[0])
        swap_copy(second).wait()
        for momentum in range(2):
            out_ref[momentum] += jnp.where(chosen[second] == momentum, 0.0, incoming[second])

    near_first = jnp.logical_or(me == 0, jnp.logical_and(lax.rem(me, 4) == 0, me >= 8))

    @pl.when(near_first)
    def _():
        def near_rest():
            near_step(steps - 3)

            @pl.when(me != 0)
            def _():
                near_step(steps - 2)
                near_step(steps - 1)

        def far_rest():
            for piece in range(pieces - per_step, pieces):
                forward(piece)
            shape_mate(1, steps - 1)

        finish(0, 1, near_rest, far_rest)

    @pl.when(jnp.logical_not(near_first))
    def _():
        def far_rest():
            forward(pieces - 2)
            near_step(steps - 3)
            forward(pieces - 1)
            shape_mate(1, steps - 1)
            near_step(steps - 2)

        finish(1, 0, far_rest, lambda: near_step(steps - 1))

    energy_far().wait_send()
    energy_near(False).wait_send()

    @pl.when(me == 1)
    def _():
        sent(own_raw.at[core, :, pl.ds(0, virtuals - LAST * PIECE)], near_send.at[0])

    @pl.when(me != 1)
    def _():
        sent(own_raw.at[core], near_send.at[0])

    @pl.when(jnp.logical_or(me == ring - 1, me == ring - 4))
    def _():
        sent(side, side_send.at[0])

    for slot in range(MOST):
        @pl.when(jnp.logical_and(carrier, slot < lent(me + 2)))
        def _():
            loan_carry(slot).wait_send()


def fused(factors, occupied_energy, virtual_energy, conserve, pair_lists):
    momenta, orbitals, virtuals, parts, auxiliary = factors.shape
    ring = lax.axis_size("ka")
    pieces = virtuals // PIECE
    bands = virtuals // BAND
    half = virtuals // 2
    tiles = pl.cdiv(virtuals, LANES)
    packed = (half * 2 * tiles, LANES)
    dma = pltpu.SemaphoreType.DMA
    density = pl.pallas_call(
        functools.partial(fused_kernel, ring, virtuals, auxiliary),
        out_shape=pltpu.VMEM((momenta, *packed), jnp.float32),
        in_specs=[
            pl.BlockSpec(memory_space=pltpu.HBM),
            pl.BlockSpec(memory_space=pltpu.HBM),
            pl.BlockSpec(memory_space=pltpu.HBM),
            pl.BlockSpec(memory_space=pltpu.HBM),
        ],
        out_specs=pl.BlockSpec(memory_space=pltpu.VMEM),
        scratch_shapes=[
            pltpu.SMEM(conserve.shape, conserve.dtype),
            pltpu.SMEM(occupied_energy.shape, occupied_energy.dtype),
            pltpu.VMEM(virtual_energy.shape, virtual_energy.dtype),
            pltpu.VMEM((momenta, orbitals, virtuals, parts, auxiliary), jnp.bfloat16),
            pltpu.VMEM((2, orbitals, virtuals, parts, auxiliary), jnp.bfloat16),
            pltpu.VMEM((LAST, orbitals, PIECE, parts, auxiliary), jnp.bfloat16),
            pltpu.VMEM((MOST, orbitals, PIECE, parts, auxiliary), jnp.bfloat16),
            pltpu.VMEM((momenta, orbitals * virtuals, parts * auxiliary), jnp.bfloat16),
            pltpu.VMEM((2, bands, orbitals * 2 * BAND, parts * auxiliary), jnp.bfloat16),
            pltpu.VMEM((2, momenta, virtuals), jnp.bfloat16),
            pltpu.VMEM((momenta, virtuals, LANES), jnp.float32),
            pltpu.VMEM((2, bands, 3, virtuals, LANES), jnp.float32),
            pltpu.VMEM((orbitals * virtuals, orbitals * 2 * BAND), jnp.float32),
            pltpu.VMEM((2, 2, virtuals, tiles * LANES), jnp.float32),
            pltpu.VMEM((2, *packed), jnp.float32),
            pltpu.VMEM((2, *packed), jnp.float32),
            dma((3,)), dma((2,)),
            dma((1,)), dma((pieces,)), dma((1,)), dma((virtuals // STEP,)),
            dma((2,)), dma((2,)), dma((2,)), dma((2,)),
            dma((1,)), dma((LAST,)), dma((MOST,)), dma((MOST,)),
        ],
        compiler_params=pltpu.CompilerParams(
            collective_id=0, has_side_effects=True, vmem_limit_bytes=54 * 1024 * 1024
        ),
        name="density",
    )(conserve, occupied_energy, virtual_energy, factors)
    split = density.reshape(momenta, half, tiles, 2, LANES).transpose(0, 1, 3, 2, 4)
    return split.reshape(momenta, half, 2, tiles * LANES)[..., :virtuals]


def local(factors, occupied_energy, virtual_energy, conserve, pair_lists):
    momenta, orbitals, virtuals, parts, auxiliary = factors.shape
    rounds, pairs = pair_lists.shape[:2]
    ring, holders = lax.axis_size("ka"), lax.axis_size("occ")
    whole_square = pairs * holders == orbitals * orbitals
    fits = momenta == 2 and orbitals == 2 and holders == 2 and rounds == 2
    even = ring % 4 == 0 and ring > 8 and auxiliary % LANES == 0
    banded = virtuals % BAND == 0 and virtuals >= 2 * BAND
    chosen = fused if whole_square and fits and even and banded else general
    return chosen(factors, occupied_energy, virtual_energy, conserve, pair_lists)


def solution(mesh):
    in_specs = (
        P("ka", None, None, None, None),
        P(),
        P("ka", None),
        P("ka", None),
        P(None, "occ", None),
    )
    out_specs = P("ka", "occ", None, None)
    return jax.shard_map(local, mesh=mesh, in_specs=in_specs, out_specs=out_specs, check_vma=False)
```

```python
import functools

import jax
import jax.numpy as jnp
from jax import lax
from jax.experimental import pallas as pl
from jax.experimental.pallas import tpu as pltpu
from jax.sharding import PartitionSpec as P

LANES = 128
BAND = 64
STEP = 16
PIECE = 8
LAST = 4
MOST = 2


def from_behind(array, axis, by):
    size = lax.axis_size(axis)
    return lax.ppermute(array, axis, [(i, (i + by) % size) for i in range(size)])


def build_mates(received, auxiliary):
    real_part = received[..., :auxiliary]
    imaginary = received[..., auxiliary:]
    turned = jnp.concatenate([-imaginary, real_part], axis=-1)
    return jnp.concatenate([received, turned], axis=-2)


def amplitude(left_rows, mate_rows, energy_left, energy_right, occupied_sum):
    values = lax.dot_general(
        left_rows, mate_rows, (((1,), (1,)), ((), ())), preferred_element_type=jnp.float32
    )
    denominator = energy_left[:, None] + energy_right[None, :] - occupied_sum
    return values / jnp.concatenate([denominator, denominator], axis=1)


def density_term(amplitudes, swapped):
    virtuals = amplitudes.shape[0]
    combined = (2.0 * amplitudes - swapped).astype(jnp.bfloat16)
    rounded = amplitudes.astype(jnp.bfloat16)
    turned = jnp.concatenate([-rounded[:, virtuals:], rounded[:, :virtuals]], axis=1)
    stacked = jnp.concatenate([rounded, turned], axis=0)
    return lax.dot_general(
        combined, stacked, (((1,), (1,)), ((), ())), preferred_element_type=jnp.float32
    )


def pair_term(own_block, mate_block, energy_left, energy_right, occupied_energy, pair_row):
    leading = pair_row[0]
    trailing = pair_row[1]
    occupied_sum = occupied_energy[leading] + occupied_energy[trailing]
    amplitudes = amplitude(
        own_block[leading], mate_block[trailing], energy_left, energy_right, occupied_sum
    )
    swapped = amplitude(
        own_block[trailing], mate_block[leading], energy_left, energy_right, occupied_sum
    )
    return density_term(amplitudes, swapped)


def general(factors, occupied_energy, virtual_energy, conserve, pair_lists):
    momenta = factors.shape[0]
    orbitals = factors.shape[1]
    virtuals = factors.shape[2]
    auxiliary = factors.shape[4]
    own = factors.reshape(momenta, orbitals, virtuals, 2 * auxiliary)
    energy_own = virtual_energy.astype(jnp.float32)
    density = jnp.zeros((momenta, virtuals, 2 * virtuals), jnp.float32)
    for round_index in range(conserve.shape[1]):
        portion = orbitals // lax.axis_size("occ")
        portion_block = lax.dynamic_slice_in_dim(
            factors, lax.axis_index("occ") * portion, portion, 1
        )
        shifted, energy_mate = from_behind((portion_block, virtual_energy), "ka", round_index + 1)
        received = lax.all_gather(shifted, "occ", axis=1, tiled=True)
        mates = build_mates(received.reshape(momenta, orbitals, virtuals, 2 * auxiliary), auxiliary)
        energy_mate = energy_mate.astype(jnp.float32)
        for local_index in range(momenta):
            chosen = (momenta - conserve[local_index, round_index] % momenta) % momenta
            mate_block = lax.dynamic_index_in_dim(mates, chosen, 0, keepdims=False)
            energy_right = lax.dynamic_index_in_dim(energy_mate, chosen, 0, keepdims=False)
            own_block = own[local_index]
            energy_left = energy_own[local_index]

            def add_pair(partial_sum, pair_row):
                term = pair_term(
                    own_block, mate_block, energy_left, energy_right, occupied_energy, pair_row
                )
                return (partial_sum + term, None)

            running, ignored = lax.scan(add_pair, density[local_index], pair_lists[round_index])
            density = density.at[local_index].set(running)
    shaped = density.reshape(momenta, virtuals, 2, virtuals)
    return lax.psum_scatter(shaped, "occ", scatter_dimension=1, tiled=True)


def fused_kernel(
    ring, virtuals, auxiliary,
    conserve_hbm, occupied_hbm, energy_hbm, factors_ref, out_ref,
    conserve_ref, occupied_ref, energy_ref, own_raw, mate_raw, side, own, mate, energy_in, energy_left, inverse, products, right_rows, total, outgoing, incoming, partial,
    small_sem, own_sem, far_send, far_recv, near_send, near_recv,
    energy_send, energy_recv, swap_send, swap_recv, side_send, side_recv,
):
    mesh_id = pl.DeviceIdType.MESH
    me = lax.axis_index("ka")
    core = lax.axis_index("occ")
    other = 1 - core
    odd = lax.rem(me, 2)
    half = virtuals // 2
    pieces = virtuals // PIECE
    steps = virtuals // STEP
    bands = virtuals // BAND
    per_step = STEP // PIECE
    per_band = BAND // STEP
    tiles = pl.cdiv(virtuals, LANES)
    stride = 2 * tiles

    def at(step):
        return lax.rem(me + step + ring, ring)

    near = at(1 - 2 * odd)
    lender = jnp.logical_and(lax.rem(me, 4) == 2, me != ring - 2)
    carrier = jnp.logical_and(lax.rem(me, 4) == 0, me != ring - 4)

    def lent(sender):
        return jnp.where(sender == ring - 6, MOST, 2)

    def keeps(piece):
        return jnp.logical_or(jnp.logical_not(lender), piece < pieces - lent(me))

    def sent(done, semaphore):
        pltpu.make_async_copy(done, done, semaphore).wait()

    def own_copy(momentum):
        return pltpu.make_async_copy(
            factors_ref.at[momentum], own_raw.at[momentum], own_sem.at[0]
        )

    def small_copies():
        return (
            pltpu.make_async_copy(conserve_hbm, conserve_ref, small_sem.at[0]),
            pltpu.make_async_copy(occupied_hbm, occupied_ref, small_sem.at[1]),
            pltpu.make_async_copy(energy_hbm, energy_ref, small_sem.at[2]),
        )

    barrier = pltpu.get_barrier_semaphore()
    for place in ((at(-2), core), (near, core), (me, other)):
        pl.semaphore_signal(barrier, inc=1, device_id=place, device_id_type=mesh_id)
    for listener, speaker in ((0, ring - 4), (ring - 4, ring - 1)):
        @pl.when(me == listener)
        def _():
            pl.semaphore_signal(
                barrier, inc=1, device_id=(speaker, core), device_id_type=mesh_id
            )

    @pl.when(carrier)
    def _():
        pl.semaphore_signal(barrier, inc=1, device_id=(at(2), core), device_id_type=mesh_id)

    @pl.when(jnp.logical_and(lax.rem(me, 4) == 0, me != 0))
    def _():
        pl.semaphore_signal(barrier, inc=1, device_id=(at(-4), core), device_id_type=mesh_id)

    own_copy(core).start()
    for copy in small_copies():
        copy.start()
    own_copy(other).start()

    def piece_rows(piece):
        return pl.ds(pl.multiple_of(piece * PIECE, PIECE), PIECE)

    def step_rows(step):
        return pl.ds(pl.multiple_of(step * STEP, STEP), STEP)

    def far_copy(piece):
        return pltpu.make_async_remote_copy(
            src_ref=factors_ref.at[core, :, piece_rows(piece)],
            dst_ref=mate_raw.at[1, :, piece_rows(piece)],
            send_sem=far_send.at[0], recv_sem=far_recv.at[piece],
            device_id=(at(2), core), device_id_type=mesh_id,
        )

    def near_copy(piece, relay):
        source = mate_raw.at[1] if relay else factors_ref.at[core]
        return pltpu.make_async_remote_copy(
            src_ref=source.at[:, piece_rows(piece)],
            dst_ref=mate_raw.at[0, :, piece_rows(piece)],
            send_sem=near_send.at[0], recv_sem=near_recv.at[piece // per_step],
            device_id=(near, core), device_id_type=mesh_id,
        )

    def near_arrival(step):
        rows = mate_raw.at[0, :, step_rows(step)]
        return pltpu.make_async_copy(rows, rows, near_recv.at[step])

    def lend_copy(slot):
        piece = pieces - LAST + slot
        return pltpu.make_async_remote_copy(
            src_ref=factors_ref.at[core, :, piece_rows(piece)], dst_ref=side.at[slot],
            send_sem=side_send.at[0], recv_sem=side_recv.at[slot],
            device_id=(ring - 4, core), device_id_type=mesh_id,
        )

    def carry_copy(slot):
        piece = pieces - LAST + slot
        return pltpu.make_async_remote_copy(
            src_ref=side.at[slot], dst_ref=mate_raw.at[0, :, piece_rows(piece)],
            send_sem=side_send.at[0], recv_sem=near_recv.at[piece // per_step],
            device_id=(0, core), device_id_type=mesh_id,
        )

    def loan_copy(slot):
        return pltpu.make_async_remote_copy(
            src_ref=factors_ref.at[core, :, piece_rows(pieces - lent(me) + slot)],
            dst_ref=side.at[slot],
            send_sem=far_send.at[0], recv_sem=side_recv.at[slot],
            device_id=(at(-2), core), device_id_type=mesh_id,
        )

    def loan_carry(slot):
        piece = pieces - lent(me + 2) + slot
        return pltpu.make_async_remote_copy(
            src_ref=side.at[slot], dst_ref=mate_raw.at[1, :, piece_rows(piece)],
            send_sem=side_send.at[0], recv_sem=far_recv.at[piece],
            device_id=(at(4), core), device_id_type=mesh_id,
        )

    def energy_far():
        return pltpu.make_async_remote_copy(
            src_ref=energy_ref, dst_ref=energy_in.at[1],
            send_sem=energy_send.at[0], recv_sem=energy_recv.at[1],
            device_id=(at(2), core), device_id_type=mesh_id,
        )

    def energy_near(relay):
        return pltpu.make_async_remote_copy(
            src_ref=energy_in.at[1] if relay else energy_ref, dst_ref=energy_in.at[0],
            send_sem=energy_send.at[0], recv_sem=energy_recv.at[0],
            device_id=(near, core), device_id_type=mesh_id,
        )

    extra = jnp.logical_or(jnp.logical_or(lender, carrier), me >= ring - 1)
    greeters = jnp.where(jnp.logical_or(extra, me == ring - 4), 4, 3)
    pl.semaphore_wait(barrier, greeters)

    @pl.when(me == ring - 1)
    def _():
        for slot in range(LAST):
            lend_copy(slot).start()

    for slot in range(MOST):
        @pl.when(jnp.logical_and(lender, slot < lent(me)))
        def _():
            loan_copy(slot).start()

    late = me == ring - 6

    def send_far(piece, carry):
        @pl.when(keeps(piece))
        def _():
            far_copy(piece).start()

        return carry

    def send_piece(piece, carry):
        @pl.when(jnp.logical_not(late))
        def _():
            send_far(piece, 0)

        @pl.when(odd == 0)
        def _():
            near_copy(piece, False).start()

        return carry

    lax.fori_loop(0, 2, send_piece, 0)
    for copy in small_copies():
        copy.wait()
    energy_far().start()

    @pl.when(odd == 0)
    def _():
        energy_near(False).start()

    lax.fori_loop(2, pieces, send_piece, 0)

    chosen = []
    for slot in range(2):
        mirror = lax.rem(2 - lax.rem(conserve_ref[0, slot], 2), 2)
        chosen.append(jnp.where(mirror == core, 0, 1))

    sent(own_raw, own_sem.at[0])

    def forward(piece):
        far_copy(piece).wait_recv()

        @pl.when(jnp.logical_and(odd == 1, jnp.logical_or(me != 1, piece < pieces - LAST)))
        def _():
            near_copy(piece, True).start()

    def shape_own(step, carry):
        for momentum in range(2):
            for orbital in range(2):
                row = pl.ds(pl.multiple_of(orbital * virtuals + step * STEP, STEP), STEP)
                raw = own_raw[momentum, orbital, step_rows(step)]
                own[momentum, row, :] = raw.reshape(STEP, 2 * auxiliary)
        return carry

    def shape_mate(slot, step):
        band = step // per_band
        for orbital in range(2):
            both = mate_raw[slot, orbital, step_rows(step)].reshape(STEP, 2 * auxiliary)
            real, imaginary = both[:, :auxiliary], both[:, auxiliary:]
            first = orbital * 2 * BAND + lax.rem(step, per_band) * STEP
            plain = pl.ds(pl.multiple_of(first, STEP), STEP)
            turned = pl.ds(pl.multiple_of(first + BAND, STEP), STEP)
            mate[slot, band, plain, pl.ds(0, auxiliary)] = real
            mate[slot, band, plain, pl.ds(auxiliary, auxiliary)] = imaginary
            mate[slot, band, turned, pl.ds(0, auxiliary)] = -imaginary
            mate[slot, band, turned, pl.ds(auxiliary, auxiliary)] = real

    def shape_energies():
        sums = [occupied_ref[0] + occupied_ref[0], occupied_ref[0] + occupied_ref[1]]
        sums.append(occupied_ref[1] + occupied_ref[1])
        diagonal = lax.broadcasted_iota(
            jnp.int32, (virtuals, virtuals), 0
        ) == lax.broadcasted_iota(jnp.int32, (virtuals, virtuals), 1)
        mine = energy_ref[...].astype(jnp.float32)
        for momentum in range(2):
            spread = jnp.where(diagonal, mine[momentum : momentum + 1, :], 0.0)
            column = jnp.sum(spread, axis=1, keepdims=True)
            energy_left[momentum] = jnp.broadcast_to(column, (virtuals, LANES))
        energy_near(False).wait_recv()
        for slot in range(2):
            theirs = energy_in[slot].astype(jnp.float32)
            theirs = jnp.where(core == 0, theirs[0:1, :], theirs[1:2, :])
            for band in range(bands):
                part = theirs[:, band * BAND : (band + 1) * BAND]
                row = jnp.concatenate([part, part], axis=1)
                base = energy_left[chosen[slot]] + row
                for kind in range(3):
                    inverse[slot, band, kind] = 1.0 / (base - sums[kind])

    sign = jnp.where(lax.broadcasted_iota(jnp.int32, (virtuals, LANES), 1) < BAND, -1.0, 1.0)

    def amplitude_of(slot, band, i, j, start, rows):
        value = products[slot, pl.ds(i * virtuals + start, rows), j * LANES : (j + 1) * LANES]
        return value * inverse[slot, band, i + j, pl.ds(start, rows), :]

    def band_products(slot, band):
        momentum = jnp.where(slot == 1, chosen[1], chosen[0])
        products[slot] = lax.dot_general(
            own[momentum], mate[slot, band], (((1,), (1,)), ((), ())),
            preferred_element_type=jnp.float32,
        )

    def band_right(slot, band):
        rounded, turned = [], []
        for i in range(2):
            for j in range(2):
                this = amplitude_of(slot, band, i, j, 0, virtuals)
                rounded.append(this.astype(jnp.bfloat16))
                turned.append((pltpu.roll(this, BAND, 1) * sign).astype(jnp.bfloat16))
        kinds = [jnp.concatenate(kind, axis=1) for kind in (rounded, turned)]
        blocks = [
            kind[start : start + LANES] for start in range(0, virtuals, LANES) for kind in kinds
        ]
        return jnp.concatenate(blocks, axis=0)

    def band_left(slot, band, start, rows):
        this = {}
        for i in range(2):
            for j in range(2):
                this[i, j] = amplitude_of(slot, band, i, j, start, rows)
        combined = [
            (2.0 * this[i, j] - this[j, i]).astype(jnp.bfloat16) for i in range(2) for j in range(2)
        ]
        return jnp.concatenate(combined, axis=1)

    def times(left, right):
        return lax.dot_general(
            left, right, (((1,), (1,)), ((), ())), preferred_element_type=jnp.float32
        )

    def add_band(slot, band):
        band_products(slot, band)
        left = band_left(slot, band, 0, virtuals)
        total[slot] += times(left, band_right(slot, band))

    def near_step(step):
        near_arrival(step).wait()
        shape_mate(0, step)

    total[...] = jnp.zeros_like(total)
    early = steps - (BAND // PIECE - 1)
    lax.fori_loop(0, early, shape_own, 0)

    def main_step(piece, carry):
        @pl.when(jnp.logical_and(carrier, piece == jnp.where(me == 0, 6, pieces - 3)))
        def _():
            for slot in range(MOST):
                @pl.when(slot < lent(me + 2))
                def _():
                    loan_copy(slot).wait_recv()
                    loan_carry(slot).start()

        forward(piece)

        @pl.when(jnp.logical_and(late, piece == 1))
        def _():
            lax.fori_loop(0, pieces, send_far, 0)

        for slot in range(LAST):
            @pl.when(jnp.logical_and(me == ring - 4, piece == slot + 8))
            def _():
                lend_copy(slot).wait_recv()
                carry_copy(slot).start()

        for behind in (1, 2):
            @pl.when(jnp.logical_and(me == 0, piece == pieces - 5 - 2 * behind))
            def _():
                near_step(steps - behind)

        @pl.when(piece == 1)
        def _():
            energy_far().wait_recv()

            @pl.when(odd == 1)
            def _():
                energy_near(True).start()

        even_piece = lax.rem(piece, 2) == 0

        @pl.when(lax.rem(piece, per_step) == per_step - 1)
        def _():
            shape_mate(1, piece // per_step)

        lag = 4

        @pl.when(jnp.logical_and(even_piece, piece >= lag))
        def _():
            near_step((piece - lag) // 2)

        @pl.when(piece < steps - early)
        def _():
            shape_own(early + piece, 0)

        @pl.when(piece == steps - early)
        def _():
            shape_energies()

        phase = lax.rem(piece, BAND // PIECE)
        ready = jnp.logical_and(piece >= BAND // PIECE, jnp.logical_or(phase == 0, phase == 3))

        @pl.when(ready)
        def _():
            add_band(jnp.where(phase == 0, 1, 0), piece // (BAND // PIECE) - 1)

        return carry

    lax.fori_loop(0, pieces - per_step, main_step, 0)

    def swap_copy(slot):
        return pltpu.make_async_remote_copy(
            src_ref=outgoing.at[slot], dst_ref=incoming.at[slot],
            send_sem=swap_send.at[0], recv_sem=swap_recv.at[slot],
            device_id=(me, other), device_id_type=mesh_id,
        )

    def half_rows(which):
        return pl.ds(pl.multiple_of(which * half, half), half)

    def spots(part, tile):
        return pl.ds(tile * 2 + part, half, stride)

    def rows_of(slot, which):
        start = pl.multiple_of(which * half, half)
        left = band_left(slot, bands - 1, start, half)
        return total[slot, pl.ds(start, half), :] + times(left, right_rows[slot])

    def own_half(slot, keep):
        known = rows_of(slot, core)
        for momentum in range(2):
            mine = jnp.where(chosen[slot] == momentum, known, 0.0)
            partial[momentum] = partial[momentum] + mine if keep else mine

    def send_half(slot, apart):
        def multiply():
            band_products(slot, bands - 1)
            right_rows[slot] = band_right(slot, bands - 1)
            outgoing[slot] = rows_of(slot, other)

        if apart:
            pl.when(core >= 0)(multiply)
        else:
            multiply()
        swap_copy(slot).start()

    def close_band(slot, keep, later):
        send_half(slot, len(later) > 0)

        @pl.when(core >= 0)
        def _():
            own_half(slot, keep)
            for behind in later:
                own_half(behind, True)

    def store_out(momentum, value):
        for tile in range(tiles):
            first = value[:, 2 * tile * LANES : (2 * tile + 1) * LANES]
            out_ref[momentum, spots(0, tile), :] = first
            if (tile + 1) * LANES <= virtuals:
                second = value[:, (2 * tile + 1) * LANES : (2 * tile + 2) * LANES]
            else:
                second = pltpu.roll(first, LANES // 2, 1)
            out_ref[momentum, spots(1, tile), :] = second

    def finish(first, second, before_first, before_second, together):
        def theirs(slot, momentum):
            return jnp.where(chosen[slot] == momentum, 0.0, incoming[slot])

        before_first()
        if together:
            send_half(first, True)
        else:
            close_band(first, False, ())
        before_second()
        close_band(second, not together, (first,) if together else ())
        sent(own_raw.at[core], far_send.at[0])
        swap_copy(first).wait_recv()
        for momentum in range(2):
            partial[momentum] += theirs(first, momentum)
        swap_copy(second).wait_recv()
        for momentum in range(2):
            store_out(momentum, partial[momentum] + theirs(second, momentum))

    near_first = me == 0

    @pl.when(near_first)
    def _():
        def far_rest():
            for piece in range(pieces - per_step, pieces):
                forward(piece)
            shape_mate(1, steps - 1)

        def near_rest():
            @pl.when(me == 0)
            def _():
                near_step(steps - 3)

            @pl.when(me != 0)
            def _():
                near_step(steps - 2)
                far_rest()
                near_step(steps - 1)

        finish(0, 1, near_rest, lambda: pl.when(me == 0)(far_rest), True)

    @pl.when(jnp.logical_not(near_first))
    def _():
        def far_rest():
            forward(pieces - 2)
            near_step(steps - 3)
            forward(pieces - 1)
            shape_mate(1, steps - 1)
            near_step(steps - 2)

        finish(1, 0, far_rest, lambda: near_step(steps - 1), False)

    sent(energy_in, energy_send.at[0])
    sent(outgoing, swap_send.at[0])

    @pl.when(me == 1)
    def _():
        sent(own_raw.at[core, :, pl.ds(0, virtuals - LAST * PIECE)], near_send.at[0])

    @pl.when(me != 1)
    def _():
        sent(own_raw.at[core], near_send.at[0])

    @pl.when(jnp.logical_or(me == ring - 1, me == ring - 4))
    def _():
        sent(side, side_send.at[0])

    for count in (MOST,):
        @pl.when(jnp.logical_and(carrier, lent(me + 2) == count))
        def _():
            sent(side.at[pl.ds(0, count)], side_send.at[0])


def fused(factors, occupied_energy, virtual_energy, conserve, pair_lists):
    momenta, orbitals, virtuals, parts, auxiliary = factors.shape
    ring = lax.axis_size("ka")
    pieces = virtuals // PIECE
    bands = virtuals // BAND
    half = virtuals // 2
    tiles = pl.cdiv(virtuals, LANES)
    packed = (half * 2 * tiles, LANES)
    dma = pltpu.SemaphoreType.DMA
    density = pl.pallas_call(
        functools.partial(fused_kernel, ring, virtuals, auxiliary),
        out_shape=pltpu.VMEM((momenta, *packed), jnp.float32),
        in_specs=[
            pl.BlockSpec(memory_space=pltpu.HBM),
            pl.BlockSpec(memory_space=pltpu.HBM),
            pl.BlockSpec(memory_space=pltpu.HBM),
            pl.BlockSpec(memory_space=pltpu.HBM),
        ],
        out_specs=pl.BlockSpec(memory_space=pltpu.VMEM),
        scratch_shapes=[
            pltpu.SMEM(conserve.shape, conserve.dtype),
            pltpu.SMEM(occupied_energy.shape, occupied_energy.dtype),
            pltpu.VMEM(virtual_energy.shape, virtual_energy.dtype),
            pltpu.VMEM((momenta, orbitals, virtuals, parts, auxiliary), jnp.bfloat16),
            pltpu.VMEM((2, orbitals, virtuals, parts, auxiliary), jnp.bfloat16),
            pltpu.VMEM((LAST, orbitals, PIECE, parts, auxiliary), jnp.bfloat16),
            pltpu.VMEM((momenta, orbitals * virtuals, parts * auxiliary), jnp.bfloat16),
            pltpu.VMEM((2, bands, orbitals * 2 * BAND, parts * auxiliary), jnp.bfloat16),
            pltpu.VMEM((2, momenta, virtuals), jnp.bfloat16),
            pltpu.VMEM((momenta, virtuals, LANES), jnp.float32),
            pltpu.VMEM((2, bands, 3, virtuals, LANES), jnp.float32),
            pltpu.VMEM((2, orbitals * virtuals, orbitals * 2 * BAND), jnp.float32),
            pltpu.VMEM((2, 2 * virtuals, orbitals * orbitals * LANES), jnp.bfloat16),
            pltpu.VMEM((2, virtuals, 2 * virtuals), jnp.float32),
            pltpu.VMEM((2, half, 2 * virtuals), jnp.float32),
            pltpu.VMEM((2, half, 2 * virtuals), jnp.float32),
            pltpu.VMEM((2, half, 2 * virtuals), jnp.float32),
            dma((3,)), dma((1,)),
            dma((1,)), dma((pieces,)), dma((1,)), dma((virtuals // STEP,)),
            dma((1,)), dma((2,)), dma((1,)), dma((2,)),
            dma((1,)), dma((LAST,)),
        ],
        compiler_params=pltpu.CompilerParams(
            collective_id=0, has_side_effects=True, vmem_limit_bytes=54 * 1024 * 1024
        ),
        name="density",
    )(conserve, occupied_energy, virtual_energy, factors)
    split = density.reshape(momenta, half, tiles, 2, LANES).transpose(0, 1, 3, 2, 4)
    return split.reshape(momenta, half, 2, tiles * LANES)[..., :virtuals]


def local(factors, occupied_energy, virtual_energy, conserve, pair_lists):
    momenta, orbitals, virtuals, parts, auxiliary = factors.shape
    rounds, pairs = pair_lists.shape[:2]
    ring, holders = lax.axis_size("ka"), lax.axis_size("occ")
    whole_square = pairs * holders == orbitals * orbitals
    fits = momenta == 2 and orbitals == 2 and holders == 2 and rounds == 2
    even = ring % 4 == 0 and ring > 8 and auxiliary % LANES == 0
    banded = virtuals % BAND == 0 and virtuals >= 2 * BAND
    chosen = fused if whole_square and fits and even and banded else general
    return chosen(factors, occupied_energy, virtual_energy, conserve, pair_lists)


def solution(mesh):
    in_specs = (
        P("ka", None, None, None, None),
        P(),
        P("ka", None),
        P("ka", None),
        P(None, "occ", None),
    )
    out_specs = P("ka", "occ", None, None)
    return jax.shard_map(local, mesh=mesh, in_specs=in_specs, out_specs=out_specs, check_vma=False)
```

```python
import functools

import jax
import jax.numpy as jnp
from jax import lax
from jax.experimental import pallas as pl
from jax.experimental.pallas import tpu as pltpu
from jax.sharding import PartitionSpec as P

LANES = 128
BAND = 64
STEP = 16
PIECE = 8
LAST = 4
MOST = 2


def from_behind(array, axis, by):
    size = lax.axis_size(axis)
    return lax.ppermute(array, axis, [(i, (i + by) % size) for i in range(size)])


def build_mates(received, auxiliary):
    real_part = received[..., :auxiliary]
    imaginary = received[..., auxiliary:]
    turned = jnp.concatenate([-imaginary, real_part], axis=-1)
    return jnp.concatenate([received, turned], axis=-2)


def amplitude(left_rows, mate_rows, energy_left, energy_right, occupied_sum):
    values = lax.dot_general(
        left_rows, mate_rows, (((1,), (1,)), ((), ())), preferred_element_type=jnp.float32
    )
    denominator = energy_left[:, None] + energy_right[None, :] - occupied_sum
    return values / jnp.concatenate([denominator, denominator], axis=1)


def density_term(amplitudes, swapped):
    virtuals = amplitudes.shape[0]
    combined = (2.0 * amplitudes - swapped).astype(jnp.bfloat16)
    rounded = amplitudes.astype(jnp.bfloat16)
    turned = jnp.concatenate([-rounded[:, virtuals:], rounded[:, :virtuals]], axis=1)
    stacked = jnp.concatenate([rounded, turned], axis=0)
    return lax.dot_general(
        combined, stacked, (((1,), (1,)), ((), ())), preferred_element_type=jnp.float32
    )


def pair_term(own_block, mate_block, energy_left, energy_right, occupied_energy, pair_row):
    leading = pair_row[0]
    trailing = pair_row[1]
    occupied_sum = occupied_energy[leading] + occupied_energy[trailing]
    amplitudes = amplitude(
        own_block[leading], mate_block[trailing], energy_left, energy_right, occupied_sum
    )
    swapped = amplitude(
        own_block[trailing], mate_block[leading], energy_left, energy_right, occupied_sum
    )
    return density_term(amplitudes, swapped)


def general(factors, occupied_energy, virtual_energy, conserve, pair_lists):
    momenta = factors.shape[0]
    orbitals = factors.shape[1]
    virtuals = factors.shape[2]
    auxiliary = factors.shape[4]
    own = factors.reshape(momenta, orbitals, virtuals, 2 * auxiliary)
    energy_own = virtual_energy.astype(jnp.float32)
    density = jnp.zeros((momenta, virtuals, 2 * virtuals), jnp.float32)
    for round_index in range(conserve.shape[1]):
        portion = orbitals // lax.axis_size("occ")
        portion_block = lax.dynamic_slice_in_dim(
            factors, lax.axis_index("occ") * portion, portion, 1
        )
        shifted, energy_mate = from_behind((portion_block, virtual_energy), "ka", round_index + 1)
        received = lax.all_gather(shifted, "occ", axis=1, tiled=True)
        mates = build_mates(received.reshape(momenta, orbitals, virtuals, 2 * auxiliary), auxiliary)
        energy_mate = energy_mate.astype(jnp.float32)
        for local_index in range(momenta):
            chosen = (momenta - conserve[local_index, round_index] % momenta) % momenta
            mate_block = lax.dynamic_index_in_dim(mates, chosen, 0, keepdims=False)
            energy_right = lax.dynamic_index_in_dim(energy_mate, chosen, 0, keepdims=False)
            own_block = own[local_index]
            energy_left = energy_own[local_index]

            def add_pair(partial_sum, pair_row):
                term = pair_term(
                    own_block, mate_block, energy_left, energy_right, occupied_energy, pair_row
                )
                return (partial_sum + term, None)

            running, ignored = lax.scan(add_pair, density[local_index], pair_lists[round_index])
            density = density.at[local_index].set(running)
    shaped = density.reshape(momenta, virtuals, 2, virtuals)
    return lax.psum_scatter(shaped, "occ", scatter_dimension=1, tiled=True)


def fused_kernel(
    ring, virtuals, auxiliary,
    conserve_hbm, occupied_hbm, energy_hbm, factors_ref, out_ref,
    conserve_ref, occupied_ref, energy_ref, own_raw, mate_raw, side, own, mate, energy_in, energy_left, inverse, products, right_rows, total, outgoing, incoming, partial,
    small_sem, own_sem, far_send, far_recv, near_send, near_recv,
    energy_send, energy_recv, swap_send, swap_recv, side_send, side_recv,
):
    mesh_id = pl.DeviceIdType.MESH
    me = lax.axis_index("ka")
    core = lax.axis_index("occ")
    other = 1 - core
    odd = lax.rem(me, 2)
    half = virtuals // 2
    pieces = virtuals // PIECE
    steps = virtuals // STEP
    bands = virtuals // BAND
    per_step = STEP // PIECE
    per_band = BAND // STEP
    tiles = pl.cdiv(virtuals, LANES)
    stride = 2 * tiles

    def at(step):
        return lax.rem(me + step + ring, ring)

    near = at(1 - 2 * odd)
    lender = jnp.logical_and(lax.rem(me, 4) == 2, me != ring - 2)
    carrier = jnp.logical_and(lax.rem(me, 4) == 0, me != ring - 4)

    def lent(sender):
        return jnp.where(sender == ring - 6, MOST, 2)

    def keeps(piece):
        return jnp.logical_or(jnp.logical_not(lender), piece < pieces - lent(me))

    def sent(done, semaphore):
        pltpu.make_async_copy(done, done, semaphore).wait()

    def own_copy(momentum):
        return pltpu.make_async_copy(
            factors_ref.at[momentum], own_raw.at[momentum], own_sem.at[0]
        )

    def small_copies():
        return (
            pltpu.make_async_copy(conserve_hbm, conserve_ref, small_sem.at[0]),
            pltpu.make_async_copy(occupied_hbm, occupied_ref, small_sem.at[1]),
            pltpu.make_async_copy(energy_hbm, energy_ref, small_sem.at[2]),
        )

    barrier = pltpu.get_barrier_semaphore()
    for place in ((at(-2), core), (near, core), (me, other)):
        pl.semaphore_signal(barrier, inc=1, device_id=place, device_id_type=mesh_id)
    for listener, speaker in ((0, ring - 4), (ring - 4, ring - 1)):
        @pl.when(me == listener)
        def _():
            pl.semaphore_signal(
                barrier, inc=1, device_id=(speaker, core), device_id_type=mesh_id
            )

    @pl.when(carrier)
    def _():
        pl.semaphore_signal(barrier, inc=1, device_id=(at(2), core), device_id_type=mesh_id)

    @pl.when(jnp.logical_and(lax.rem(me, 4) == 0, me != 0))
    def _():
        pl.semaphore_signal(barrier, inc=1, device_id=(at(-4), core), device_id_type=mesh_id)

    own_copy(core).start()
    for copy in small_copies():
        copy.start()
    own_copy(other).start()

    def near_slot(step):
        paired = (steps - 4) // 2
        return jnp.where(step < steps - 4, step // 2, step - (steps - 4) + paired)

    def piece_rows(piece):
        return pl.ds(pl.multiple_of(piece * PIECE, PIECE), PIECE)

    def step_rows(step):
        return pl.ds(pl.multiple_of(step * STEP, STEP), STEP)

    def far_copy(piece):
        return pltpu.make_async_remote_copy(
            src_ref=factors_ref.at[core, :, piece_rows(piece)],
            dst_ref=mate_raw.at[1, :, piece_rows(piece)],
            send_sem=far_send.at[0], recv_sem=far_recv.at[piece],
            device_id=(at(2), core), device_id_type=mesh_id,
        )

    def near_copy(piece, relay):
        source = mate_raw.at[1] if relay else factors_ref.at[core]
        return pltpu.make_async_remote_copy(
            src_ref=source.at[:, piece_rows(piece)],
            dst_ref=mate_raw.at[0, :, piece_rows(piece)],
            send_sem=near_send.at[0], recv_sem=near_recv.at[near_slot(piece // per_step)],
            device_id=(near, core), device_id_type=mesh_id,
        )

    def near_arrival(step, count):
        rows = mate_raw.at[0, :, pl.ds(pl.multiple_of(step * STEP, STEP), count * STEP)]
        return pltpu.make_async_copy(rows, rows, near_recv.at[near_slot(step)])

    def lend_copy(slot):
        piece = pieces - LAST + slot
        return pltpu.make_async_remote_copy(
            src_ref=factors_ref.at[core, :, piece_rows(piece)], dst_ref=side.at[slot],
            send_sem=side_send.at[0], recv_sem=side_recv.at[slot],
            device_id=(ring - 4, core), device_id_type=mesh_id,
        )

    def carry_copy(slot):
        piece = pieces - LAST + slot
        return pltpu.make_async_remote_copy(
            src_ref=side.at[slot], dst_ref=mate_raw.at[0, :, piece_rows(piece)],
            send_sem=side_send.at[0], recv_sem=near_recv.at[near_slot(piece // per_step)],
            device_id=(0, core), device_id_type=mesh_id,
        )

    def loan_copy(slot):
        return pltpu.make_async_remote_copy(
            src_ref=factors_ref.at[core, :, piece_rows(pieces - lent(me) + slot)],
            dst_ref=side.at[slot],
            send_sem=far_send.at[0], recv_sem=side_recv.at[slot],
            device_id=(at(-2), core), device_id_type=mesh_id,
        )

    def loan_carry(slot):
        piece = pieces - lent(me + 2) + slot
        return pltpu.make_async_remote_copy(
            src_ref=side.at[slot], dst_ref=mate_raw.at[1, :, piece_rows(piece)],
            send_sem=side_send.at[0], recv_sem=far_recv.at[piece],
            device_id=(at(4), core), device_id_type=mesh_id,
        )

    def energy_far():
        return pltpu.make_async_remote_copy(
            src_ref=energy_ref, dst_ref=energy_in.at[1],
            send_sem=energy_send.at[0], recv_sem=energy_recv.at[1],
            device_id=(at(2), core), device_id_type=mesh_id,
        )

    def energy_near(relay):
        return pltpu.make_async_remote_copy(
            src_ref=energy_in.at[1] if relay else energy_ref, dst_ref=energy_in.at[0],
            send_sem=energy_send.at[0], recv_sem=energy_recv.at[0],
            device_id=(near, core), device_id_type=mesh_id,
        )

    extra = jnp.logical_or(jnp.logical_or(lender, carrier), me >= ring - 1)
    greeters = jnp.where(jnp.logical_or(extra, me == ring - 4), 4, 3)
    pl.semaphore_wait(barrier, greeters)

    @pl.when(me == ring - 1)
    def _():
        for slot in range(LAST):
            lend_copy(slot).start()

    for slot in range(MOST):
        @pl.when(jnp.logical_and(lender, slot < lent(me)))
        def _():
            loan_copy(slot).start()

    late = me == ring - 6

    def send_far(piece, carry):
        @pl.when(keeps(piece))
        def _():
            far_copy(piece).start()

        return carry

    def send_piece(piece, carry):
        @pl.when(jnp.logical_not(late))
        def _():
            send_far(piece, 0)

        @pl.when(odd == 0)
        def _():
            near_copy(piece, False).start()

        return carry

    lax.fori_loop(0, 2, send_piece, 0)
    for copy in small_copies():
        copy.wait()
    energy_far().start()

    @pl.when(odd == 0)
    def _():
        energy_near(False).start()

    lax.fori_loop(2, pieces, send_piece, 0)

    chosen = []
    for slot in range(2):
        mirror = lax.rem(2 - lax.rem(conserve_ref[0, slot], 2), 2)
        chosen.append(jnp.where(mirror == core, 0, 1))

    sent(own_raw, own_sem.at[0])

    def forward(piece):
        far_copy(piece).wait_recv()

        @pl.when(jnp.logical_and(odd == 1, jnp.logical_or(me != 1, piece < pieces - LAST)))
        def _():
            near_copy(piece, True).start()

    def shape_own(step, carry):
        for momentum in range(2):
            for orbital in range(2):
                row = pl.ds(pl.multiple_of(orbital * virtuals + step * STEP, STEP), STEP)
                raw = own_raw[momentum, orbital, step_rows(step)]
                own[momentum, row, :] = raw.reshape(STEP, 2 * auxiliary)
        return carry

    def shape_mate(slot, step):
        band = step // per_band
        for orbital in range(2):
            both = mate_raw[slot, orbital, step_rows(step)].reshape(STEP, 2 * auxiliary)
            real, imaginary = both[:, :auxiliary], both[:, auxiliary:]
            first = orbital * 2 * BAND + lax.rem(step, per_band) * STEP
            plain = pl.ds(pl.multiple_of(first, STEP), STEP)
            turned = pl.ds(pl.multiple_of(first + BAND, STEP), STEP)
            mate[slot, band, plain, pl.ds(0, auxiliary)] = real
            mate[slot, band, plain, pl.ds(auxiliary, auxiliary)] = imaginary
            mate[slot, band, turned, pl.ds(0, auxiliary)] = -imaginary
            mate[slot, band, turned, pl.ds(auxiliary, auxiliary)] = real

    def shape_energies():
        sums = [occupied_ref[0] + occupied_ref[0], occupied_ref[0] + occupied_ref[1]]
        sums.append(occupied_ref[1] + occupied_ref[1])
        diagonal = lax.broadcasted_iota(
            jnp.int32, (virtuals, virtuals), 0
        ) == lax.broadcasted_iota(jnp.int32, (virtuals, virtuals), 1)
        mine = energy_ref[...].astype(jnp.float32)
        for momentum in range(2):
            spread = jnp.where(diagonal, mine[momentum : momentum + 1, :], 0.0)
            column = jnp.sum(spread, axis=1, keepdims=True)
            energy_left[momentum] = jnp.broadcast_to(column, (virtuals, LANES))
        energy_near(False).wait_recv()
        for slot in range(2):
            theirs = energy_in[slot].astype(jnp.float32)
            theirs = jnp.where(core == 0, theirs[0:1, :], theirs[1:2, :])
            for band in range(bands):
                part = theirs[:, band * BAND : (band + 1) * BAND]
                row = jnp.concatenate([part, part], axis=1)
                base = energy_left[chosen[slot]] + row
                for kind in range(3):
                    inverse[slot, band, kind] = 1.0 / (base - sums[kind])

    sign = jnp.where(lax.broadcasted_iota(jnp.int32, (virtuals, LANES), 1) < BAND, -1.0, 1.0)

    def amplitude_of(slot, band, i, j, start, rows):
        value = products[slot, pl.ds(i * virtuals + start, rows), j * LANES : (j + 1) * LANES]
        return value * inverse[slot, band, i + j, pl.ds(start, rows), :]

    def band_products(slot, band):
        momentum = jnp.where(slot == 1, chosen[1], chosen[0])
        products[slot] = lax.dot_general(
            own[momentum], mate[slot, band], (((1,), (1,)), ((), ())),
            preferred_element_type=jnp.float32,
        )

    def band_right(slot, band):
        rounded, turned = [], []
        for i in range(2):
            for j in range(2):
                this = amplitude_of(slot, band, i, j, 0, virtuals)
                rounded.append(this.astype(jnp.bfloat16))
                turned.append((pltpu.roll(this, BAND, 1) * sign).astype(jnp.bfloat16))
        kinds = [jnp.concatenate(kind, axis=1) for kind in (rounded, turned)]
        blocks = [
            kind[start : start + LANES] for start in range(0, virtuals, LANES) for kind in kinds
        ]
        return jnp.concatenate(blocks, axis=0)

    def band_left(slot, band, start, rows):
        this = {}
        for i in range(2):
            for j in range(2):
                this[i, j] = amplitude_of(slot, band, i, j, start, rows)
        combined = [
            (2.0 * this[i, j] - this[j, i]).astype(jnp.bfloat16) for i in range(2) for j in range(2)
        ]
        return jnp.concatenate(combined, axis=1)

    def times(left, right):
        return lax.dot_general(
            left, right, (((1,), (1,)), ((), ())), preferred_element_type=jnp.float32
        )

    def add_band(slot, band):
        band_products(slot, band)
        left = band_left(slot, band, 0, virtuals)
        total[slot] += times(left, band_right(slot, band))

    def near_step(step):
        @pl.when(jnp.logical_and(step < steps - 4, lax.rem(step, 2) == 0))
        def _():
            near_arrival(step, 2).wait()

        @pl.when(jnp.asarray(step >= steps - 4))
        def _():
            near_arrival(step, 1).wait()

        shape_mate(0, step)

    total[...] = jnp.zeros_like(total)
    early = steps - (BAND // PIECE - 1)
    lax.fori_loop(0, early, shape_own, 0)

    def main_step(piece, carry):
        @pl.when(jnp.logical_and(carrier, piece == jnp.where(me == 0, 6, pieces - 3)))
        def _():
            for slot in range(MOST):
                @pl.when(slot < lent(me + 2))
                def _():
                    loan_copy(slot).wait_recv()
                    loan_carry(slot).start()

        forward(piece)

        @pl.when(jnp.logical_and(late, piece == 1))
        def _():
            lax.fori_loop(0, pieces, send_far, 0)

        for slot in range(LAST):
            @pl.when(jnp.logical_and(me == ring - 4, piece == slot + 8))
            def _():
                lend_copy(slot).wait_recv()
                carry_copy(slot).start()

        for behind in (1, 2):
            @pl.when(jnp.logical_and(me == 0, piece == pieces - 5 - 2 * behind))
            def _():
                near_step(steps - behind)

        @pl.when(piece == 1)
        def _():
            energy_far().wait_recv()

            @pl.when(odd == 1)
            def _():
                energy_near(True).start()

        even_piece = lax.rem(piece, 2) == 0

        @pl.when(lax.rem(piece, per_step) == per_step - 1)
        def _():
            shape_mate(1, piece // per_step)

        lag = 4

        @pl.when(jnp.logical_and(even_piece, piece >= lag))
        def _():
            near_step((piece - lag) // 2)

        @pl.when(piece < steps - early)
        def _():
            shape_own(early + piece, 0)

        @pl.when(piece == steps - early)
        def _():
            shape_energies()

        phase = lax.rem(piece, BAND // PIECE)
        ready = jnp.logical_and(piece >= BAND // PIECE, jnp.logical_or(phase == 0, phase == 3))

        @pl.when(ready)
        def _():
            add_band(jnp.where(phase == 0, 1, 0), piece // (BAND // PIECE) - 1)

        return carry

    lax.fori_loop(0, pieces - per_step, main_step, 0)

    def swap_copy(slot):
        return pltpu.make_async_remote_copy(
            src_ref=outgoing.at[slot], dst_ref=incoming.at[slot],
            send_sem=swap_send.at[0], recv_sem=swap_recv.at[slot],
            device_id=(me, other), device_id_type=mesh_id,
        )

    def half_rows(which):
        return pl.ds(pl.multiple_of(which * half, half), half)

    def spots(part, tile):
        return pl.ds(tile * 2 + part, half, stride)

    def rows_of(slot, which):
        start = pl.multiple_of(which * half, half)
        left = band_left(slot, bands - 1, start, half)
        return total[slot, pl.ds(start, half), :] + times(left, right_rows[slot])

    def own_half(slot, keep):
        known = rows_of(slot, core)
        for momentum in range(2):
            mine = jnp.where(chosen[slot] == momentum, known, 0.0)
            partial[momentum] = partial[momentum] + mine if keep else mine

    def send_half(slot, apart):
        def multiply():
            band_products(slot, bands - 1)
            right_rows[slot] = band_right(slot, bands - 1)
            outgoing[slot] = rows_of(slot, other)

        if apart:
            pl.when(core >= 0)(multiply)
        else:
            multiply()
        swap_copy(slot).start()

    def close_band(slot, keep, later):
        send_half(slot, len(later) > 0)

        @pl.when(core >= 0)
        def _():
            own_half(slot, keep)
            for behind in later:
                own_half(behind, True)

    def store_out(momentum, value):
        for tile in range(tiles):
            first = value[:, 2 * tile * LANES : (2 * tile + 1) * LANES]
            out_ref[momentum, spots(0, tile), :] = first
            if (tile + 1) * LANES <= virtuals:
                second = value[:, (2 * tile + 1) * LANES : (2 * tile + 2) * LANES]
            else:
                second = pltpu.roll(first, LANES // 2, 1)
            out_ref[momentum, spots(1, tile), :] = second

    def finish(first, second, before_first, before_second, together):
        def theirs(slot, momentum):
            return jnp.where(chosen[slot] == momentum, 0.0, incoming[slot])

        before_first()
        if together:
            send_half(first, True)
        else:
            close_band(first, False, ())
        before_second()
        close_band(second, not together, (first,) if together else ())
        sent(own_raw.at[core], far_send.at[0])
        swap_copy(first).wait_recv()
        for momentum in range(2):
            partial[momentum] += theirs(first, momentum)
        swap_copy(second).wait_recv()
        for momentum in range(2):
            store_out(momentum, partial[momentum] + theirs(second, momentum))

    near_first = me == 0

    @pl.when(near_first)
    def _():
        def far_rest():
            for piece in range(pieces - per_step, pieces):
                forward(piece)
            shape_mate(1, steps - 1)

        def near_rest():
            @pl.when(me == 0)
            def _():
                near_step(steps - 3)

            @pl.when(me != 0)
            def _():
                near_step(steps - 2)
                far_rest()
                near_step(steps - 1)

        finish(0, 1, near_rest, lambda: pl.when(me == 0)(far_rest), True)

    @pl.when(jnp.logical_not(near_first))
    def _():
        def far_rest():
            forward(pieces - 2)
            near_step(steps - 3)
            forward(pieces - 1)
            shape_mate(1, steps - 1)
            near_step(steps - 2)

        finish(1, 0, far_rest, lambda: near_step(steps - 1), False)

    sent(energy_in, energy_send.at[0])
    sent(outgoing, swap_send.at[0])

    @pl.when(me == 1)
    def _():
        sent(own_raw.at[core, :, pl.ds(0, virtuals - LAST * PIECE)], near_send.at[0])

    @pl.when(me != 1)
    def _():
        sent(own_raw.at[core], near_send.at[0])

    @pl.when(jnp.logical_or(me == ring - 1, me == ring - 4))
    def _():
        sent(side, side_send.at[0])

    for count in (MOST,):
        @pl.when(jnp.logical_and(carrier, lent(me + 2) == count))
        def _():
            sent(side.at[pl.ds(0, count)], side_send.at[0])


def fused(factors, occupied_energy, virtual_energy, conserve, pair_lists):
    momenta, orbitals, virtuals, parts, auxiliary = factors.shape
    ring = lax.axis_size("ka")
    pieces = virtuals // PIECE
    bands = virtuals // BAND
    half = virtuals // 2
    tiles = pl.cdiv(virtuals, LANES)
    packed = (half * 2 * tiles, LANES)
    dma = pltpu.SemaphoreType.DMA
    density = pl.pallas_call(
        functools.partial(fused_kernel, ring, virtuals, auxiliary),
        out_shape=pltpu.VMEM((momenta, *packed), jnp.float32),
        in_specs=[
            pl.BlockSpec(memory_space=pltpu.HBM),
            pl.BlockSpec(memory_space=pltpu.HBM),
            pl.BlockSpec(memory_space=pltpu.HBM),
            pl.BlockSpec(memory_space=pltpu.HBM),
        ],
        out_specs=pl.BlockSpec(memory_space=pltpu.VMEM),
        scratch_shapes=[
            pltpu.SMEM(conserve.shape, conserve.dtype),
            pltpu.SMEM(occupied_energy.shape, occupied_energy.dtype),
            pltpu.VMEM(virtual_energy.shape, virtual_energy.dtype),
            pltpu.VMEM((momenta, orbitals, virtuals, parts, auxiliary), jnp.bfloat16),
            pltpu.VMEM((2, orbitals, virtuals, parts, auxiliary), jnp.bfloat16),
            pltpu.VMEM((LAST, orbitals, PIECE, parts, auxiliary), jnp.bfloat16),
            pltpu.VMEM((momenta, orbitals * virtuals, parts * auxiliary), jnp.bfloat16),
            pltpu.VMEM((2, bands, orbitals * 2 * BAND, parts * auxiliary), jnp.bfloat16),
            pltpu.VMEM((2, momenta, virtuals), jnp.bfloat16),
            pltpu.VMEM((momenta, virtuals, LANES), jnp.float32),
            pltpu.VMEM((2, bands, 3, virtuals, LANES), jnp.float32),
            pltpu.VMEM((2, orbitals * virtuals, orbitals * 2 * BAND), jnp.float32),
            pltpu.VMEM((2, 2 * virtuals, orbitals * orbitals * LANES), jnp.bfloat16),
            pltpu.VMEM((2, virtuals, 2 * virtuals), jnp.float32),
            pltpu.VMEM((2, half, 2 * virtuals), jnp.float32),
            pltpu.VMEM((2, half, 2 * virtuals), jnp.float32),
            pltpu.VMEM((2, half, 2 * virtuals), jnp.float32),
            dma((3,)), dma((1,)),
            dma((1,)), dma((pieces,)), dma((1,)), dma((virtuals // STEP // 2 + 2,)),
            dma((1,)), dma((2,)), dma((1,)), dma((2,)),
            dma((1,)), dma((LAST,)),
        ],
        compiler_params=pltpu.CompilerParams(
            collective_id=0, has_side_effects=True, vmem_limit_bytes=54 * 1024 * 1024,
        ),
        name="density",
    )(conserve, occupied_energy, virtual_energy, factors)
    split = density.reshape(momenta, half, tiles, 2, LANES).transpose(0, 1, 3, 2, 4)
    return split.reshape(momenta, half, 2, tiles * LANES)[..., :virtuals]


def local(factors, occupied_energy, virtual_energy, conserve, pair_lists):
    momenta, orbitals, virtuals, parts, auxiliary = factors.shape
    rounds, pairs = pair_lists.shape[:2]
    ring, holders = lax.axis_size("ka"), lax.axis_size("occ")
    whole_square = pairs * holders == orbitals * orbitals
    fits = momenta == 2 and orbitals == 2 and holders == 2 and rounds == 2
    even = ring % 4 == 0 and ring > 8 and auxiliary % LANES == 0
    banded = virtuals % BAND == 0 and virtuals >= 2 * BAND
    chosen = fused if whole_square and fits and even and banded else general
    return chosen(factors, occupied_energy, virtual_energy, conserve, pair_lists)


def solution(mesh):
    in_specs = (
        P("ka", None, None, None, None),
        P(),
        P("ka", None),
        P("ka", None),
        P(None, "occ", None),
    )
    out_specs = P("ka", "occ", None, None)
    return jax.shard_map(local, mesh=mesh, in_specs=in_specs, out_specs=out_specs, check_vma=False)
```
